32 devices in a mesh: qrow: 4 (over y, x), kcol: 8 (over z, core).
Axes of the slice: x: 2, y: 2, z: 4, core: 2. Of those that a mesh axis runs over, the one named last changes fastest.
Arguments:
- queries: bfloat16 [8192, 512], P(('qrow', 'kcol')), may hold values from -6 to 6
- keys: bfloat16 [8192, 128], P(('kcol', 'qrow')), may hold values from -6 to 6
- values: bfloat16 [8192, 128], P(('kcol', 'qrow')), may hold values from -6 to 6
- block_mask: int32 [64, 64], replicated, may hold values from 0 to 1, as said below
Outputs:
- attended: float32 [8192, 512], P(('qrow', 'kcol'))
The draws below stay inside these ranges and needn't reach their ends.
Inputs may be any that keep to these rules, and one draw needn't show every extreme that they name: block_mask[a, b] is 1 only where b <= a, and always where 0 <= a - b < 3.
All inputs are finite; a program needn't handle non-finite values.
Results may differ from the reference program's by a relative error of at most 0.0022.
Values may be sent and summed in bfloat16 or wider, within the bound.
A program may use at most 64 MiB of HBM per device.

```python
import math
import jax
import jax.numpy as jnp
from jax import lax

H = 4
DH = 128
BLOCK = 128
QBT = 16
S = 8192
NB = 64


def draw_queries(key, part):
    base_rows = jnp.clip(jax.random.normal(jax.random.fold_in(key, 11), (S, H * DH)), -6.0, 6.0)
    return base_rows.astype(jnp.bfloat16)


def draw_keys(key, part):
    base_rows = jnp.clip(jax.random.normal(jax.random.fold_in(key, 12), (S, DH)), -6.0, 6.0)
    return base_rows.astype(jnp.bfloat16)


def draw_block_mask(key, part):
    row_ids = jnp.arange(NB, dtype=jnp.int32)[:, None]
    col_ids = jnp.arange(NB, dtype=jnp.int32)[None, :]
    distance = row_ids - col_ids
    picks = jax.random.randint(jax.random.fold_in(key, 14), (NB, NB), 0, 100)
    semantic = (col_ids % 2 == 0) & (picks < 55)
    listed = (distance >= 0) & ((distance < 3) | semantic | (picks < 15))
    return listed.astype(jnp.int32)


def level_of(key, extent, cuts, smallest, top_value):
    gain = 1.0
    for axis_at, blocks in cuts:
        draws = jax.random.uniform(jax.random.fold_in(jax.random.fold_in(key, 6), axis_at), (blocks,), jnp.float32, smallest / len(cuts), top_value / len(cuts))
        gain = gain * jnp.repeat(jnp.exp(draws), extent[axis_at] // blocks).reshape((-1,) + (1,) * (len(extent) - 1 - axis_at))
    return gain


def noise(own_key, shape, scale, most, split=(), kind=jnp.bfloat16):
    level = level_of(own_key, shape, split, -0.22, 0.18) if split else 1.0
    entries = jax.random.normal(own_key, shape, jnp.float32) * scale * level
    return jnp.minimum(jnp.maximum(entries, -most), most).astype(kind)


def setup_inputs(seed: int = 0) -> dict:
    key_list = jax.random.split(jax.random.key(seed), 5)
    return {
        "queries": draw_queries(jax.random.fold_in(key_list[4], 71), 0),
        "keys": draw_keys(jax.random.fold_in(key_list[4], 71), 0),
        "values": noise(key_list[2], (S, DH), 1.0, 6.0, ((0, 32),)),
        "block_mask": draw_block_mask(jax.random.fold_in(key_list[4], 71), 0),
    }


NEG_FILL = -1e+30

def reference(queries, keys, values, block_mask):
    inv_root = 1.0 / math.sqrt(DH)
    query_wide = queries.astype(jnp.float32)
    key_wide = keys.astype(jnp.float32)
    value_wide = values.astype(jnp.float32)
    group_rows = QBT * BLOCK
    pieces = []
    for group in range(S // group_rows):
        end_tok = (group + 1) * group_rows
        end_blk = end_tok // BLOCK
        key_part = key_wide[:end_tok]
        value_part = value_wide[:end_tok].reshape(end_blk, BLOCK, DH)
        key_pos = jnp.arange(end_tok, dtype=jnp.int32)

        def one_block(block_index, key_part=key_part, value_part=value_part, key_pos=key_pos, end_blk=end_blk):
            first_row = block_index * BLOCK
            query_heads = lax.dynamic_slice_in_dim(query_wide, first_row, BLOCK, 0).reshape(BLOCK, H, DH)
            scores = jnp.einsum('rhd,kd->hrk', query_heads, key_part, precision=lax.Precision.HIGHEST) * inv_root
            mask_row = lax.dynamic_index_in_dim(block_mask, block_index, 0, keepdims=False)[:end_blk]
            listed = jnp.repeat(mask_row, BLOCK) == 1
            query_pos = first_row + jnp.arange(BLOCK, dtype=jnp.int32)
            permitted = listed[None, :] & (key_pos[None, :] <= query_pos[:, None])
            permitted = permitted.reshape(BLOCK, end_blk, BLOCK)
            scores = scores.reshape(H, BLOCK, end_blk, BLOCK)
            scores = jnp.where(permitted[None], scores, NEG_FILL)
            block_top = lax.optimization_barrier(jnp.max(scores, axis=3))
            weights = jnp.where(permitted[None], jnp.exp(scores - block_top[..., None]), 0.0).astype(jnp.bfloat16)
            weights_wide = weights.astype(jnp.float32)
            block_mass = lax.optimization_barrier(jnp.sum(weights_wide, axis=3))
            block_out = jnp.einsum('hrkb,kbd->hrkd', weights_wide, value_part, precision=lax.Precision.HIGHEST)
            row_top = lax.optimization_barrier(jnp.max(block_top, axis=2))
            factor = jnp.exp(block_top - row_top[..., None])
            numerator = lax.optimization_barrier(jnp.sum(block_out * factor[..., None], axis=2))
            denominator = lax.optimization_barrier(jnp.sum(block_mass * factor, axis=2))
            mixed = numerator / denominator[..., None]
            return jnp.transpose(mixed, (1, 0, 2)).reshape(BLOCK, H * DH)
        first_blk = group * group_rows // BLOCK
        outs_group = lax.map(one_block, jnp.arange(first_blk, end_blk, dtype=jnp.int32))
        pieces.append(outs_group.reshape(group_rows, H * DH))
    return jnp.concatenate(pieces, axis=0)
```

```python
import math

import jax
import jax.numpy as jnp
from jax import lax
from jax.experimental import pallas as pl
from jax.experimental.pallas import tpu as pltpu
from jax.sharding import PartitionSpec as P

H = 4
DH = 128
BLOCK = 128
SIZES = (16, 8, 4)
NEAR = 3
TILE = 256
BIG = 4e30
MOST = 64
NEG_FILL = -1e30
SCALE = math.log2(math.e) / math.sqrt(DH)


def attend(mask_ref, q_ref, k_ref, v_ref, out_ref, listed, flipped, total, mass, top, held, sent):
    tokens = q_ref.shape[0]
    part = min(tokens, BLOCK)
    pieces_here = tokens // part
    width = H * part
    tiles = pieces_here * width // TILE
    last = mask_ref.shape[1] - 1
    device = lax.axis_index("qrow") * lax.axis_size("kcol") + lax.axis_index("kcol")
    firsts = [device * tokens + own * part for own in range(pieces_here)]
    rows = [first // BLOCK for first in firsts]

    def rows_of(ref, block):
        return ref[pl.ds(pl.multiple_of(block * BLOCK, BLOCK), BLOCK), :]

    for own in range(pieces_here):
        turned = jnp.concatenate(
            [
                q_ref[own * part : (own + 1) * part, h * DH : (h + 1) * DH].T
                for h in range(H)
            ],
            axis=1,
        )
        scaled = turned.astype(jnp.float32) * SCALE
        coarse = scaled.astype(jnp.bfloat16)
        at = slice(own * width, (own + 1) * width)
        flipped[:DH, at] = coarse
        flipped[DH:, at] = (scaled - coarse.astype(jnp.float32)).astype(jnp.bfloat16)

    total[...] = jnp.zeros_like(total)
    mass[...] = jnp.zeros_like(mass)
    top[...] = jnp.full_like(top, NEG_FILL)

    def attend_to(lists, diagonal):
        keys, flipped_values = [], []
        for blocks, _ in lists:
            rows_in = jnp.concatenate([rows_of(k_ref, b) for b in blocks], axis=0)
            keys.append(jnp.concatenate([rows_in, rows_in], axis=1))
            seen = jnp.concatenate([rows_of(v_ref, b) for b in blocks], axis=0)
            ones = jnp.ones((16, seen.shape[0]), jnp.bfloat16)
            flipped_values.append(jnp.concatenate([seen.T, ones], axis=0))

        def scores_of(t):
            columns = slice(t * TILE, (t + 1) * TILE)
            return jnp.dot(
                keys[t * TILE // width], flipped[:, columns], preferred_element_type=jnp.float32
            )

        def weigh(t, scores):
            columns = slice(t * TILE, (t + 1) * TILE)
            _, absent = lists[t * TILE // width]
            pieces = [scores[g * BLOCK : (g + 1) * BLOCK] for g in range(len(absent))]
            if diagonal:
                key_at = lax.broadcasted_iota(jnp.int32, pieces[0].shape, 0)
                query_at = lax.broadcasted_iota(jnp.int32, pieces[0].shape, 1) % part
                query_at = query_at + firsts[t * TILE // width] % BLOCK
                pieces[0] = jnp.where(key_at <= query_at, pieces[0], -BIG)
            old = top[:, columns]
            new = old
            for piece, off in zip(pieces, absent):
                new = jnp.maximum(new, jnp.max(piece, axis=0, keepdims=True) - off)
            top[:, columns] = new
            weights = [
                jnp.exp2(piece - (new + off)).astype(jnp.bfloat16)
                for piece, off in zip(pieces, absent)
            ]
            return jnp.exp2(old - new), jnp.concatenate(weights, axis=0)

        def gather(t, fade, weights):
            columns = slice(t * TILE, (t + 1) * TILE)
            summed = jnp.dot(
                flipped_values[t * TILE // width], weights, preferred_element_type=jnp.float32
            )
            mass[:, columns] = mass[:, columns] * fade + summed[DH : DH + 1]
            total[:, columns] = total[:, columns] * fade + summed[:DH]

        scores, held_back = scores_of(0), None
        for t in range(tiles):
            ahead = scores_of(t + 1) if t + 1 < tiles else None
            weighed = weigh(t, scores)
            if held_back is not None:
                gather(t - 1, *held_back)
            scores, held_back = ahead, weighed
        gather(tiles - 1, *held_back)

    def penalty(here):
        return jnp.where(here, 0.0, BIG).astype(jnp.float32)

    attend_to(
        [
            (
                [jnp.maximum(row - back, 0) for back in range(NEAR)],
                [penalty(row >= back) for back in range(NEAR)],
            )
            for row in rows
        ],
        True,
    )

    def note(i, counts):
        found = []
        for own, (row, count) in enumerate(zip(rows, counts)):
            j = last - i
            listed[own, count] = j
            far = (j + NEAR <= row).astype(jnp.int32)
            found.append(count + far * mask_ref[row, j])
        return tuple(found)

    counts = lax.fori_loop(
        0, last + 1, note, tuple(jnp.int32(0) for _ in rows), unroll=16
    )
    most = counts[0]
    for count in counts[1:]:
        most = jnp.maximum(most, count)
    done = jnp.int32(0)
    for size in SIZES:
        left = most - done
        trips = left // size if size > SIZES[-1] else (left + size - 1) // size

        def step(t, carried, done=done, size=size):
            start = done + t * size
            lists = []
            for own, count in enumerate(counts):
                here = [start + g < count for g in range(size)]
                blocks = [
                    jnp.where(here[g], listed[own, jnp.minimum(start + g, last)], 0)
                    for g in range(size)
                ]
                lists.append((blocks, [penalty(ok) for ok in here]))
            attend_to(lists, False)
            return carried

        lax.fori_loop(0, trips, step, 0)
        done = done + trips * size

    copies = []
    for own in range(pieces_here):
        here = pl.ds(own * part, part)
        for h in range(H):
            at = slice(own * width + h * part, own * width + (h + 1) * part)
            held[here, h * DH : (h + 1) * DH] = (total[:, at] / mass[:, at]).T
        copy = pltpu.make_async_copy(held.at[here, :], out_ref.at[here, :], sent.at[own])
        copy.start()
        copies.append(copy)
    for copy in copies:
        copy.wait()


def spread(k_ref, v_ref, k_all, v_all, send, recv, local):
    ring, lane = lax.axis_size("kcol"), lax.axis_size("qrow")
    depth, width = ring // 2, lane // 2
    q, c = lax.axis_index("qrow"), lax.axis_index("kcol")
    level, core = c // 2, c % 2
    high, low = q // width, q % width
    tokens = k_ref.shape[0]
    own, whole = (k_ref, v_ref), (k_all, v_all)
    sibling = {"qrow": q, "kcol": level * 2 + (1 - core)}
    over = {"qrow": (1 - high) * width + low, "kcol": c}
    sides = [(low + i) % width for i in range(1, width)]
    beside = [{"qrow": high * width + i, "kcol": c} for i in sides]
    up = {"qrow": q, "kcol": c + 2}
    down = {"qrow": q, "kcol": c - 2}
    has_up, has_down = level < depth - 1, level > 0

    def slot(at, column, parity=core):
        return (at * 2 + parity) * lane + column

    def place(kv, block):
        return whole[kv].at[pl.ds(pl.multiple_of(block * tokens, tokens), tokens), :]

    copies = [
        pltpu.make_async_copy(own[kv], place(kv, slot(level, q)), local.at[kv]) for kv in range(2)
    ]
    for copy in copies:
        copy.start()

    barrier = pltpu.get_barrier_semaphore()

    def greet(target):
        pl.semaphore_signal(
            barrier, inc=1, device_id=target, device_id_type=pl.DeviceIdType.MESH
        )

    for target in [sibling, over] + beside:
        greet(target)
    pl.when(has_up)(lambda: greet(up))
    pl.when(has_down)(lambda: greet(down))
    ends = has_up.astype(jnp.int32) + has_down.astype(jnp.int32)
    pl.semaphore_wait(barrier, 2 + len(beside) + ends)

    for copy in copies:
        copy.wait()
    started = []

    def landed(ok, kv, block):
        @pl.when(ok)
        def _():
            here = place(kv, block)
            pltpu.make_async_copy(here, here, recv.at[kv, block]).wait()

    def push(ok, kv, block, target, kind, at):
        copy = pltpu.make_async_remote_copy(
            src_ref=place(kv, block),
            dst_ref=place(kv, block),
            send_sem=send.at[kind, at],
            recv_sem=recv.at[kv, block],
            device_id=target,
            device_id_type=pl.DeviceIdType.MESH,
        )
        pl.when(ok)(copy.start)
        started.append((ok, copy))

    def column_sends(ok, at, way):
        block = slot(at, q)
        for kv in range(2):
            if way == 0:
                push(has_up, kv, block, up, 0 + kv, at)
                push(has_down, kv, block, down, 2 + kv, at)
            else:
                landed(ok, kv, block)
                if way > 0:
                    push(ok & has_up, kv, block, up, 0 + kv, at)
                else:
                    push(ok & has_down, kv, block, down, 2 + kv, at)
            push(ok, kv, block, over, 4 + kv, at)
            for i, target in enumerate(beside):
                push(ok, kv, block, target, 8 + 2 * i + kv, at)
            push(ok, kv, block, sibling, 6 + kv, at)

    base = 8 + 2 * len(beside)

    def relays(ok, at):
        kind = base
        for i in sides:
            block = slot(at, high * width + i)
            landed(ok, 0, block)
            push(ok, 0, block, over, kind, at)
            push(ok, 0, block, sibling, kind + 1, at)
            kind += 2
        block = slot(at, (1 - high) * width + low)
        for kv in (1, 0):
            landed(ok, kv, block)
            if kv == 1:
                for target in beside:
                    push(ok, 1, block, target, kind, at)
                    kind += 1
            push(ok, kv, block, sibling, kind, at)
            kind += 1
        for i in sides:
            block = slot(at, high * width + i)
            landed(ok, 1, block)
            push(ok, 1, block, sibling, kind, at)
            kind += 1

    last = base + 4 * len(beside) + 2

    def corners(ok, at):
        kind = last
        for i in sides:
            block = slot(at, (1 - high) * width + i)
            for kv in range(2):
                landed(ok, kv, block)
                push(ok, kv, block, sibling, kind, at)
                kind += 1

    def positions(step):
        if step == 0:
            return [(level >= 0, level, 0)]
        return [
            (level >= step, level - step, 1),
            (level + step < depth, level + step, -1),
        ]

    for step in range(depth + 2):
        if step < depth:
            for ok, at, way in positions(step):
                column_sends(ok, at, way)
        if 1 <= step <= depth:
            for ok, at, _ in positions(step - 1):
                relays(ok, at)
        if step >= 2:
            for ok, at, _ in positions(step - 2):
                corners(ok, at)
    for at in range(depth):
        for column in range(lane):
            for kv in range(2):
                landed(level >= 0, kv, slot(at, column, 1 - core))
    for ok, copy in started:
        pl.when(ok)(copy.wait_send)


def in_hbm(array):
    return pltpu.with_memory_space_constraint(array, pltpu.HBM)


def gathered(keys, values):
    ring, lane = lax.axis_size("kcol"), lax.axis_size("qrow")
    devices = ring * lane
    if ring % 2 or lane % 2 or devices > MOST:
        both = ("kcol", "qrow")
        return (
            lax.all_gather(keys, both, axis=0, tiled=True),
            lax.all_gather(values, both, axis=0, tiled=True),
        )
    vmem = pl.BlockSpec(memory_space=pltpu.VMEM)
    full = jax.ShapeDtypeStruct((keys.shape[0] * devices, keys.shape[1]), keys.dtype)
    side = lane // 2 - 1
    return pl.pallas_call(
        spread,
        out_shape=(full, full),
        in_specs=[pl.BlockSpec(memory_space=pltpu.HBM)] * 2,
        out_specs=(vmem, vmem),
        scratch_shapes=[
            pltpu.SemaphoreType.DMA((10 + 8 * side, ring // 2)),
            pltpu.SemaphoreType.DMA((2, devices)),
            pltpu.SemaphoreType.DMA((2,)),
        ],
        compiler_params=pltpu.CompilerParams(
            collective_id=0, has_side_effects=True, vmem_limit_bytes=32 * 2**20
        ),
    )(in_hbm(keys), in_hbm(values))


def shards(queries, keys, values, block_mask):
    all_keys, all_values = gathered(keys, values)
    columns = queries.shape[0] * H
    vmem = pl.BlockSpec(memory_space=pltpu.VMEM)
    return pl.pallas_call(
        attend,
        out_shape=jax.ShapeDtypeStruct(queries.shape, jnp.float32),
        in_specs=[pl.BlockSpec(memory_space=pltpu.SMEM), vmem, vmem, vmem],
        out_specs=pl.BlockSpec(memory_space=pltpu.HBM),
        scratch_shapes=[
            pltpu.SMEM((pl.cdiv(queries.shape[0], BLOCK), block_mask.shape[1]), jnp.int32),
            pltpu.VMEM((2 * DH, columns), jnp.bfloat16),
            pltpu.VMEM((DH, columns), jnp.float32),
            pltpu.VMEM((1, columns), jnp.float32),
            pltpu.VMEM((1, columns), jnp.float32),
            pltpu.VMEM(queries.shape, jnp.float32),
            pltpu.SemaphoreType.DMA((pl.cdiv(queries.shape[0], BLOCK),)),
        ],
        compiler_params=pltpu.CompilerParams(vmem_limit_bytes=48 * 2**20),
    )(in_hbm(block_mask), queries, all_keys, all_values)


def solution(mesh):
    placed = (P(("qrow", "kcol"), None), P(("kcol", "qrow"), None), P(("kcol", "qrow"), None), P())
    return jax.shard_map(
        shards, mesh=mesh, in_specs=placed, out_specs=P(("qrow", "kcol"), None), check_vma=False
    )
```

```python
import math

import jax
import jax.numpy as jnp
from jax import lax
from jax.experimental import pallas as pl
from jax.experimental.pallas import tpu as pltpu
from jax.sharding import PartitionSpec as P

H = 4
DH = 128
BLOCK = 128
SIZES = (16, 8, 4)
NEAR = 3
TILE = 256
BIG = 4e30
SQUARE = 4
SENDS = 128
NEG_FILL = -1e30
SCALE = math.log2(math.e) / math.sqrt(DH)


def attend(mask_ref, q_ref, k_ref, v_ref, out_ref, listed, flipped, total, mass, top, held, sent):
    tokens = q_ref.shape[0]
    part = min(tokens, BLOCK)
    pieces_here = tokens // part
    width = H * part
    tiles = pieces_here * width // TILE
    last = mask_ref.shape[1] - 1
    device = lax.axis_index("qrow") * lax.axis_size("kcol") + lax.axis_index("kcol")
    firsts = [device * tokens + own * part for own in range(pieces_here)]
    rows = [first // BLOCK for first in firsts]

    def rows_of(ref, block):
        return ref[pl.ds(pl.multiple_of(block * BLOCK, BLOCK), BLOCK), :]

    for own in range(pieces_here):
        turned = jnp.concatenate(
            [
                q_ref[own * part : (own + 1) * part, h * DH : (h + 1) * DH].T
                for h in range(H)
            ],
            axis=1,
        )
        scaled = turned.astype(jnp.float32) * SCALE
        coarse = scaled.astype(jnp.bfloat16)
        at = slice(own * width, (own + 1) * width)
        flipped[:DH, at] = coarse
        flipped[DH:, at] = (scaled - coarse.astype(jnp.float32)).astype(jnp.bfloat16)

    total[...] = jnp.zeros_like(total)
    mass[...] = jnp.zeros_like(mass)
    top[...] = jnp.full_like(top, NEG_FILL)

    def attend_to(lists, diagonal):
        keys, flipped_values = [], []
        for blocks, _ in lists:
            rows_in = jnp.concatenate([rows_of(k_ref, b) for b in blocks], axis=0)
            keys.append(jnp.concatenate([rows_in, rows_in], axis=1))
            seen = jnp.concatenate([rows_of(v_ref, b) for b in blocks], axis=0)
            ones = jnp.ones((16, seen.shape[0]), jnp.bfloat16)
            flipped_values.append(jnp.concatenate([seen.T, ones], axis=0))

        def scores_of(t):
            columns = slice(t * TILE, (t + 1) * TILE)
            return jnp.dot(
                keys[t * TILE // width], flipped[:, columns], preferred_element_type=jnp.float32
            )

        def weigh(t, scores):
            columns = slice(t * TILE, (t + 1) * TILE)
            _, absent = lists[t * TILE // width]
            pieces = [scores[g * BLOCK : (g + 1) * BLOCK] for g in range(len(absent))]
            if diagonal:
                key_at = lax.broadcasted_iota(jnp.int32, pieces[0].shape, 0)
                query_at = lax.broadcasted_iota(jnp.int32, pieces[0].shape, 1) % part
                query_at = query_at + firsts[t * TILE // width] % BLOCK
                pieces[0] = jnp.where(key_at <= query_at, pieces[0], -BIG)
            old = top[:, columns]
            new = old
            for piece, off in zip(pieces, absent):
                new = jnp.maximum(new, jnp.max(piece, axis=0, keepdims=True) - off)
            top[:, columns] = new
            weights = [
                jnp.exp2(piece - (new + off)).astype(jnp.bfloat16)
                for piece, off in zip(pieces, absent)
            ]
            return jnp.exp2(old - new), jnp.concatenate(weights, axis=0)

        def gather(t, fade, weights):
            columns = slice(t * TILE, (t + 1) * TILE)
            summed = jnp.dot(
                flipped_values[t * TILE // width], weights, preferred_element_type=jnp.float32
            )
            mass[:, columns] = mass[:, columns] * fade + summed[DH : DH + 1]
            total[:, columns] = total[:, columns] * fade + summed[:DH]

        scores, held_back = scores_of(0), None
        for t in range(tiles):
            ahead = scores_of(t + 1) if t + 1 < tiles else None
            weighed = weigh(t, scores)
            if held_back is not None:
                gather(t - 1, *held_back)
            scores, held_back = ahead, weighed
        gather(tiles - 1, *held_back)

    def penalty(here):
        return jnp.where(here, 0.0, BIG).astype(jnp.float32)

    attend_to(
        [
            (
                [jnp.maximum(row - back, 0) for back in range(NEAR)],
                [penalty(row >= back) for back in range(NEAR)],
            )
            for row in rows
        ],
        True,
    )

    def note(i, counts):
        found = []
        for own, (row, count) in enumerate(zip(rows, counts)):
            j = last - i
            listed[own, count] = j
            far = (j + NEAR <= row).astype(jnp.int32)
            found.append(count + far * mask_ref[row, j])
        return tuple(found)

    counts = lax.fori_loop(
        0, last + 1, note, tuple(jnp.int32(0) for _ in rows), unroll=16
    )
    most = counts[0]
    for count in counts[1:]:
        most = jnp.maximum(most, count)
    done = jnp.int32(0)
    for size in SIZES:
        left = most - done
        trips = left // size if size > SIZES[-1] else (left + size - 1) // size

        def step(t, carried, done=done, size=size):
            start = done + t * size
            lists = []
            for own, count in enumerate(counts):
                here = [start + g < count for g in range(size)]
                blocks = [
                    jnp.where(here[g], listed[own, jnp.minimum(start + g, last)], 0)
                    for g in range(size)
                ]
                lists.append((blocks, [penalty(ok) for ok in here]))
            attend_to(lists, False)
            return carried

        lax.fori_loop(0, trips, step, 0)
        done = done + trips * size

    copies = []
    for own in range(pieces_here):
        here = pl.ds(own * part, part)
        for h in range(H):
            at = slice(own * width + h * part, own * width + (h + 1) * part)
            held[here, h * DH : (h + 1) * DH] = (total[:, at] / mass[:, at]).T
        copy = pltpu.make_async_copy(held.at[here, :], out_ref.at[here, :], sent.at[own])
        copy.start()
        copies.append(copy)
    for copy in copies:
        copy.wait()


def spread(k_ref, v_ref, k_all, v_all, send, recv, local):
    ring, lane = lax.axis_size("kcol"), lax.axis_size("qrow")
    depth = ring // 2
    last = depth - 1
    q, c = lax.axis_index("qrow"), lax.axis_index("kcol")
    z, core = c // 2, c % 2
    high, low = q // 2, q % 2
    tokens = k_ref.shape[0]
    own, whole = (k_ref, v_ref), (k_all, v_all)
    beside, over = high * 2 + 1 - low, (1 - high) * 2 + low
    across = (1 - high) * 2 + 1 - low
    sibling = c + 1 - 2 * core

    def slot(plane, column, parity=core):
        return (plane * 2 + parity) * lane + column

    def place(kv, block):
        return whole[kv].at[pl.ds(pl.multiple_of(block * tokens, tokens), tokens), :]

    copies = [
        pltpu.make_async_copy(own[kv], place(kv, slot(z, q)), local.at[kv]) for kv in range(2)
    ]
    for copy in copies:
        copy.start()

    barrier = pltpu.get_barrier_semaphore()

    def greet(column, chain):
        pl.semaphore_signal(
            barrier,
            inc=1,
            device_id={"qrow": column, "kcol": chain},
            device_id_type=pl.DeviceIdType.MESH,
        )

    for step in range(1, depth):
        greet(q, (z + step) % depth * 2 + core)
    for column in (across, over, beside):
        greet(column, c)
    greet(q, sibling)
    pl.semaphore_wait(barrier, depth + lane - 1)

    for copy in copies:
        copy.wait()
    started = []

    def landed(ok, kv, block):
        @pl.when(ok)
        def _():
            here = place(kv, block)
            pltpu.make_async_copy(here, here, recv.at[kv, block]).wait()

    def push(ok, kv, block, column, chain):
        copy = pltpu.make_async_remote_copy(
            src_ref=place(kv, block),
            dst_ref=place(kv, block),
            send_sem=send.at[len(started)],
            recv_sem=recv.at[kv, block],
            device_id={"qrow": column, "kcol": chain},
            device_id_type=pl.DeviceIdType.MESH,
        )
        pl.when(ok)(copy.start)
        started.append((ok, copy))

    def wanted(column, chain, block):
        return block <= column * ring + chain

    def chip_wants(column, level, block):
        return wanted(column, level * 2 + 1, block)

    def to_sibling(ok, kv, block):
        push(ok & wanted(q, sibling, block), kv, block, q, sibling)

    def along(ok, kv, block, plane):
        for level in reversed(range(depth)):
            send_it = ok & (level != plane)
            if plane is z or plane == last:
                send_it &= (plane != last) | chip_wants(q, level, block)
            push(send_it, kv, block, q, level * 2 + core)

    def around(ok, kv, block):
        for column in (across, over, beside):
            push(ok & chip_wants(column, z, block), kv, block, column, c)

    pair = high == 1
    final = q == lane - 1
    first = z < 2
    third = z == 2
    lowest = z == last

    block = slot(z, q)
    for kv in range(2):
        push(lowest & (q < lane - 1), kv, block, lane - 1, c)
        push(third & (high == 0), kv, block, over, c)
        along(first | (third & pair) | (lowest & final), kv, block, z)
        for column in (across, over):
            push(first & chip_wants(column, z, block), kv, block, column, c)
        push((first | (third & pair)) & chip_wants(beside, z, block), kv, block, beside, c)
        to_sibling(z >= 0, kv, block)

    for kv in range(2):
        block = slot(2, q - 2)
        ok = third & pair
        landed(ok, kv, block)
        along(ok, kv, block, 2)
        push(ok & chip_wants(beside, z, block), kv, block, beside, c)
        to_sibling(ok, kv, block)
    for column in (2, 1, 0):
        for kv in range(2):
            block = slot(last, column)
            ok = lowest & final
            landed(ok, kv, block)
            along(ok, kv, block, last)
            to_sibling(ok, kv, block)

    for kv in range(2):
        for plane in (1, 0):
            block = slot(plane, q)
            ok = z != plane
            landed(ok, kv, block)
            around(ok, kv, block)
            to_sibling(ok, kv, block)
        ok = pair & (z != 2)
        for column in (q, q - 2):
            block = slot(2, column)
            landed(ok, kv, block)
            push(ok & chip_wants(beside, z, block), kv, block, beside, c)
            to_sibling(ok, kv, block)

    def ends(ok, kv, block):
        ok &= chip_wants(q, z, block)
        landed(ok, kv, block)
        to_sibling(ok, kv, block)

    for kv in range(2):
        for column in (0, 1, 2, 3):
            ends(final & (z != last), kv, slot(last, column))
    for kv in range(2):
        for column in (beside, beside - 2):
            ends(pair, kv, slot(2, column))
        for plane in (1, 0):
            for column in (beside, over, across):
                ends(z >= 0, kv, slot(plane, column))
    for plane in range(depth):
        for column in range(lane):
            for kv in range(2):
                block = slot(plane, column, 1 - core)
                landed(wanted(q, c, block), kv, block)
    for ok, copy in started:
        pl.when(ok)(copy.wait_send)


def in_hbm(array):
    return pltpu.with_memory_space_constraint(array, pltpu.HBM)


def gathered(keys, values):
    ring, lane = lax.axis_size("kcol"), lax.axis_size("qrow")
    devices = ring * lane
    if lane != SQUARE or ring != 2 * SQUARE:
        both = ("kcol", "qrow")
        return (
            lax.all_gather(keys, both, axis=0, tiled=True),
            lax.all_gather(values, both, axis=0, tiled=True),
        )
    vmem = pl.BlockSpec(memory_space=pltpu.VMEM)
    full = jax.ShapeDtypeStruct((keys.shape[0] * devices, keys.shape[1]), keys.dtype)
    return pl.pallas_call(
        spread,
        out_shape=(full, full),
        in_specs=[pl.BlockSpec(memory_space=pltpu.HBM)] * 2,
        out_specs=(vmem, vmem),
        scratch_shapes=[
            pltpu.SemaphoreType.DMA((SENDS,)),
            pltpu.SemaphoreType.DMA((2, devices)),
            pltpu.SemaphoreType.DMA((2,)),
        ],
        compiler_params=pltpu.CompilerParams(
            collective_id=0, has_side_effects=True, vmem_limit_bytes=32 * 2**20
        ),
    )(in_hbm(keys), in_hbm(values))


def shards(queries, keys, values, block_mask):
    all_keys, all_values = gathered(keys, values)
    columns = queries.shape[0] * H
    vmem = pl.BlockSpec(memory_space=pltpu.VMEM)
    return pl.pallas_call(
        attend,
        out_shape=jax.ShapeDtypeStruct(queries.shape, jnp.float32),
        in_specs=[pl.BlockSpec(memory_space=pltpu.SMEM), vmem, vmem, vmem],
        out_specs=pl.BlockSpec(memory_space=pltpu.HBM),
        scratch_shapes=[
            pltpu.SMEM((pl.cdiv(queries.shape[0], BLOCK), block_mask.shape[1]), jnp.int32),
            pltpu.VMEM((2 * DH, columns), jnp.bfloat16),
            pltpu.VMEM((DH, columns), jnp.float32),
            pltpu.VMEM((1, columns), jnp.float32),
            pltpu.VMEM((1, columns), jnp.float32),
            pltpu.VMEM(queries.shape, jnp.float32),
            pltpu.SemaphoreType.DMA((pl.cdiv(queries.shape[0], BLOCK),)),
        ],
        compiler_params=pltpu.CompilerParams(vmem_limit_bytes=48 * 2**20),
    )(in_hbm(block_mask), queries, all_keys, all_values)


def solution(mesh):
    placed = (P(("qrow", "kcol"), None), P(("kcol", "qrow"), None), P(("kcol", "qrow"), None), P())
    return jax.shard_map(
        shards, mesh=mesh, in_specs=placed, out_specs=P(("qrow", "kcol"), None), check_vma=False
    )
```

```python
import functools
import math

import jax
import jax.numpy as jnp
from jax import lax
from jax.experimental import pallas as pl
from jax.experimental.pallas import tpu as pltpu
from jax.sharding import PartitionSpec as P

H = 4
DH = 128
BLOCK = 128
SIZES = (16, 8, 4)
NEAR = 3
TILE = 256
BIG = 4e30
MOST = 64
REACH = 1
HALVES = 1
SCAN = 16
NEG_FILL = -1e30
SCALE = math.log2(math.e) / math.sqrt(DH)


def columns_of(t):
    return slice(t * TILE, (t + 1) * TILE)


def prepare(q_ref, flipped, total, mass, top):
    tokens = q_ref.shape[0]
    part = min(tokens, BLOCK)
    width = H * part
    for own in range(tokens // part):
        turned = jnp.concatenate(
            [
                q_ref[own * part : (own + 1) * part, h * DH : (h + 1) * DH].T
                for h in range(H)
            ],
            axis=1,
        )
        scaled = turned.astype(jnp.float32) * SCALE
        coarse = scaled.astype(jnp.bfloat16)
        at = slice(own * width, (own + 1) * width)
        flipped[:DH, at] = coarse
        flipped[DH:, at] = (scaled - coarse.astype(jnp.float32)).astype(jnp.bfloat16)
    total[...] = jnp.zeros_like(total)
    mass[...] = jnp.zeros_like(mass)
    top[...] = jnp.full_like(top, NEG_FILL)


def operands(key_rows, value_rows):
    ones = jnp.ones((16, value_rows.shape[0]), jnp.bfloat16)
    return (
        jnp.concatenate([key_rows, key_rows], axis=1),
        jnp.concatenate([value_rows.T, ones], axis=0),
    )


def attend_to(state, lists, width, causal=None):
    flipped, total, mass, top = state
    tiles = flipped.shape[1] // TILE

    def scores_of(t):
        keys = lists[t * TILE // width][0]
        return jnp.dot(keys, flipped[:, columns_of(t)], preferred_element_type=jnp.float32)

    def weigh(t, scores):
        columns = columns_of(t)
        absent = lists[t * TILE // width][2]
        pieces = [scores[g * BLOCK : (g + 1) * BLOCK] for g in range(len(absent))]
        if causal is not None:
            pieces[0] = causal(t, pieces[0])
        old = top[:, columns]
        new = old
        for piece, off in zip(pieces, absent):
            new = jnp.maximum(new, jnp.max(piece, axis=0, keepdims=True) - off)
        top[:, columns] = new
        weights = [
            jnp.exp2(piece - (new + off)).astype(jnp.bfloat16)
            for piece, off in zip(pieces, absent)
        ]
        return jnp.exp2(old - new), jnp.concatenate(weights, axis=0)

    def gather(t, fade, weights):
        columns = columns_of(t)
        values = lists[t * TILE // width][1]
        summed = jnp.dot(values, weights, preferred_element_type=jnp.float32)
        mass[:, columns] = mass[:, columns] * fade + summed[DH : DH + 1]
        total[:, columns] = total[:, columns] * fade + summed[:DH]

    scores, held_back = scores_of(0), None
    for t in range(tiles):
        ahead = scores_of(t + 1) if t + 1 < tiles else None
        weighed = weigh(t, scores)
        if held_back is not None:
            gather(t - 1, *held_back)
        scores, held_back = ahead, weighed
    gather(tiles - 1, *held_back)


def penalty(here):
    return jnp.where(here, 0.0, BIG).astype(jnp.float32)


def absorbed(plane, q, z):
    return (plane < q) & (plane - z <= REACH) & (z - plane <= REACH)


def attend(
    early, mask_hbm, turned, old_total, old_mass, old_top, k_ref, v_ref, out_ref,
    mask_ref, listed, total, mass, top, held, sent, fetched,
):
    fetch = pltpu.make_async_copy(mask_hbm, mask_ref, fetched.at[0])
    fetch.start()
    tokens = out_ref.shape[0]
    part = min(tokens, BLOCK)
    pieces_here = tokens // part
    width = H * part
    last = mask_ref.shape[1] - 1
    q, c = lax.axis_index("qrow"), lax.axis_index("kcol")
    device = q * lax.axis_size("kcol") + c
    plane_blocks = 2 * lax.axis_size("qrow") * tokens // BLOCK
    firsts = [device * tokens + own * part for own in range(pieces_here)]
    rows = [first // BLOCK for first in firsts]
    state = (turned, total, mass, top)
    total[...] = old_total[...]
    mass[...] = old_mass[...]
    top[...] = old_top[...]

    def gone(block):
        if not early:
            return block < 0
        return absorbed(lax.div(block, plane_blocks), q, c // 2)

    def rows_of(ref, blocks):
        return jnp.concatenate(
            [ref[pl.ds(pl.multiple_of(b * BLOCK, BLOCK), BLOCK), :] for b in blocks], axis=0
        )

    def gathered_list(blocks, absent):
        keys, values = operands(rows_of(k_ref, blocks), rows_of(v_ref, blocks))
        return keys, values, absent

    def causal(t, piece):
        key_at = lax.broadcasted_iota(jnp.int32, piece.shape, 0)
        query_at = lax.broadcasted_iota(jnp.int32, piece.shape, 1) % part
        query_at = query_at + firsts[t * TILE // width] % BLOCK
        return jnp.where(key_at <= query_at, piece, -BIG)

    near = []
    for row in rows:
        blocks = [jnp.maximum(row - back, 0) for back in range(NEAR)]
        absent = [
            penalty((row >= back) & ~gone(block)) for back, block in enumerate(blocks)
        ]
        near.append(gathered_list(blocks, absent))
    attend_to(state, near, width, causal)

    fetch.wait()

    def scan(s, counts):
        lowest = last + 1 - (s + 1) * SCAN

        def note(_, counts):
            found = list(counts)
            for i in reversed(range(SCAN)):
                j = lowest + i
                for own, row in enumerate(rows):
                    listed[own, found[own]] = j
                    far = (j + NEAR <= row).astype(jnp.int32)
                    found[own] = found[own] + far * mask_ref[row, j]
            return tuple(found)

        skip = gone(lowest) | (lowest > rows[-1])
        return lax.fori_loop(0, jnp.where(skip, 0, 1), note, counts)

    counts = lax.fori_loop(
        0, (last + 1) // SCAN, scan, tuple(jnp.int32(0) for _ in rows)
    )
    most = counts[0]
    for count in counts[1:]:
        most = jnp.maximum(most, count)
    done = jnp.int32(0)
    for size in SIZES:
        left = most - done
        trips = left // size if size > SIZES[-1] else (left + size - 1) // size

        def step(t, carried, done=done, size=size):
            start = done + t * size
            lists = []
            for own, count in enumerate(counts):
                here = [start + g < count for g in range(size)]
                blocks = [
                    jnp.where(here[g], listed[own, jnp.minimum(start + g, last)], 0)
                    for g in range(size)
                ]
                lists.append(gathered_list(blocks, [penalty(ok) for ok in here]))
            attend_to(state, lists, width)
            return carried

        lax.fori_loop(0, trips, step, 0)
        done = done + trips * size

    copies = []
    for own in range(pieces_here):
        here = pl.ds(own * part, part)
        for h in range(H):
            at = slice(own * width + h * part, own * width + (h + 1) * part)
            held[here, h * DH : (h + 1) * DH] = (total[:, at] / mass[:, at]).T
        copy = pltpu.make_async_copy(held.at[here, :], out_ref.at[here, :], sent.at[own])
        copy.start()
        copies.append(copy)
    for copy in copies:
        copy.wait()


def spread(
    q_hbm, k_ref, v_ref, mask_hbm, k_all, v_all, flipped, total, mass, top,
    q_ref, mask_ref, send, recv, local, fetched,
):
    ring, lane = lax.axis_size("kcol"), lax.axis_size("qrow")
    depth, width = ring // 2, lane // 2
    q, c = lax.axis_index("qrow"), lax.axis_index("kcol")
    level, core = c // 2, c % 2
    high, low = q // width, q % width
    tokens = k_ref.shape[0]
    own, whole = (k_ref, v_ref), (k_all, v_all)
    sibling = {"qrow": q, "kcol": level * 2 + (1 - core)}
    over = {"qrow": (1 - high) * width + low, "kcol": c}
    sides = [(low + i) % width for i in range(1, width)]
    beside = [{"qrow": high * width + i, "kcol": c} for i in sides]
    up = {"qrow": q, "kcol": c + 2}
    down = {"qrow": q, "kcol": c - 2}
    has_up, has_down = level < depth - 1, level > 0

    def slot(at, column, parity=core):
        return (at * 2 + parity) * lane + column

    def place(kv, block):
        return whole[kv].at[pl.ds(pl.multiple_of(block * tokens, tokens), tokens), :]

    copies = [
        pltpu.make_async_copy(own[kv], place(kv, slot(level, q)), local.at[kv]) for kv in range(2)
    ]
    for copy in copies:
        copy.start()

    fetches = [
        pltpu.make_async_copy(q_hbm, q_ref, fetched.at[0]),
        pltpu.make_async_copy(mask_hbm, mask_ref, fetched.at[1]),
    ]
    for fetch in fetches:
        fetch.start()

    barrier = pltpu.get_barrier_semaphore()

    def greet(target):
        pl.semaphore_signal(
            barrier, inc=1, device_id=target, device_id_type=pl.DeviceIdType.MESH
        )

    for target in [sibling, over] + beside:
        greet(target)
    pl.when(has_up)(lambda: greet(up))
    pl.when(has_down)(lambda: greet(down))
    ends = has_up.astype(jnp.int32) + has_down.astype(jnp.int32)
    pl.semaphore_wait(barrier, 2 + len(beside) + ends)

    for copy in copies:
        copy.wait()
    started = []

    def landed(ok, kv, block):
        @pl.when(ok)
        def _():
            here = place(kv, block)
            pltpu.make_async_copy(here, here, recv.at[kv, block]).wait()

    def push(ok, kv, block, target, kind, at):
        copy = pltpu.make_async_remote_copy(
            src_ref=place(kv, block),
            dst_ref=place(kv, block),
            send_sem=send.at[kind, at],
            recv_sem=recv.at[kv, block],
            device_id=target,
            device_id_type=pl.DeviceIdType.MESH,
        )
        pl.when(ok)(copy.start)
        started.append((ok, copy))

    def column_sends(ok, at, way):
        block = slot(at, q)
        for kv in range(2):
            if way == 0:
                push(has_up, kv, block, up, 0 + kv, at)
                push(has_down, kv, block, down, 2 + kv, at)
            else:
                landed(ok, kv, block)
                if way > 0:
                    push(ok & has_up, kv, block, up, 0 + kv, at)
                else:
                    push(ok & has_down, kv, block, down, 2 + kv, at)
            push(ok, kv, block, over, 4 + kv, at)
            for i, target in enumerate(beside):
                push(ok, kv, block, target, 8 + 2 * i + kv, at)
            push(ok, kv, block, sibling, 6 + kv, at)

    base = 8 + 2 * len(beside)

    def relays(ok, at):
        kind = base
        for i in sides:
            block = slot(at, high * width + i)
            landed(ok, 0, block)
            push(ok, 0, block, over, kind, at)
            push(ok, 0, block, sibling, kind + 1, at)
            kind += 2
        block = slot(at, (1 - high) * width + low)
        for kv in (1, 0):
            landed(ok, kv, block)
            if kv == 1:
                for target in beside:
                    push(ok, 1, block, target, kind, at)
                    kind += 1
            push(ok, kv, block, sibling, kind, at)
            kind += 1
        for i in sides:
            block = slot(at, high * width + i)
            landed(ok, 1, block)
            push(ok, 1, block, sibling, kind, at)
            kind += 1

    last = base + 4 * len(beside) + 2

    def corners(ok, at):
        kind = last
        for i in sides:
            block = slot(at, (1 - high) * width + i)
            for kv in range(2):
                landed(ok, kv, block)
                push(ok, kv, block, sibling, kind, at)
                kind += 1

    def positions(step):
        if step == 0:
            return [(level >= 0, level, 0)]
        return [
            (level >= step, level - step, 1),
            (level + step < depth, level + step, -1),
        ]

    state = (flipped, total, mass, top)
    part = min(q_ref.shape[0], BLOCK)
    firsts = [(q * ring + c) * q_ref.shape[0] + own for own in range(0, q_ref.shape[0], part)]
    plane_tokens = 2 * lane * tokens
    half_tokens = plane_tokens // HALVES

    def absorb(step):
        for ok, at, _ in positions(step):
            for column in range(lane):
                for kv in range(2):
                    landed(ok & (at < q), kv, slot(at, column, 1 - core))

        def half(i, carried):
            plane = jnp.where(i < HALVES, level - step, level + step)
            first = plane * plane_tokens + i % HALVES * half_tokens
            here = pl.ds(pl.multiple_of(first, half_tokens), half_tokens)
            keys, values = operands(k_all[here, :], v_all[here, :])
            lists = []
            for token in firsts:
                absent = [
                    (1 - mask_ref[token // BLOCK, first // BLOCK + g]).astype(jnp.float32) * BIG
                    for g in range(half_tokens // BLOCK)
                ]
                lists.append((keys, values, absent))
            attend_to(state, lists, H * part)
            return carried

        below = (level >= step) & (level - step < q)
        above = (level + step < depth) & (level + step < q) & (step > 0)
        lax.fori_loop(
            jnp.where(below, 0, HALVES), jnp.where(above, 2 * HALVES, HALVES), half, 0
        )

    for step in range(depth + 2):
        if step < depth:
            for ok, at, way in positions(step):
                column_sends(ok, at, way)
        if step == 0:
            for fetch in fetches:
                fetch.wait()
            prepare(q_ref, flipped, total, mass, top)
        if 1 <= step <= depth:
            for ok, at, _ in positions(step - 1):
                relays(ok, at)
        if step >= 2:
            for ok, at, _ in positions(step - 2):
                corners(ok, at)
            if step - 2 <= REACH:
                absorb(step - 2)
    for at in range(depth):
        for column in range(lane):
            for kv in range(2):
                landed(~absorbed(at, q, level), kv, slot(at, column, 1 - core))
    for ok, copy in started:
        pl.when(ok)(copy.wait_send)


def in_hbm(array):
    return pltpu.with_memory_space_constraint(array, pltpu.HBM)


def state_of(queries):
    columns = queries.shape[0] * H
    row = jax.ShapeDtypeStruct((1, columns), jnp.float32)
    return (
        jax.ShapeDtypeStruct((2 * DH, columns), jnp.bfloat16),
        jax.ShapeDtypeStruct((DH, columns), jnp.float32),
        row,
        row,
    )


def gathered(queries, keys, values, block_mask):
    ring, lane = lax.axis_size("kcol"), lax.axis_size("qrow")
    devices = ring * lane
    vmem = pl.BlockSpec(memory_space=pltpu.VMEM)
    state = state_of(queries)
    if ring != 2 * lane or lane % 2 or devices > MOST:
        both = ("kcol", "qrow")
        ready = pl.pallas_call(
            prepare, out_shape=state, in_specs=[vmem], out_specs=(vmem,) * len(state)
        )(queries)
        return False, ready, (
            lax.all_gather(keys, both, axis=0, tiled=True),
            lax.all_gather(values, both, axis=0, tiled=True),
        )
    full = jax.ShapeDtypeStruct((keys.shape[0] * devices, keys.shape[1]), keys.dtype)
    side = lane // 2 - 1
    all_keys, all_values, *ready = pl.pallas_call(
        spread,
        out_shape=(full, full) + state,
        in_specs=[pl.BlockSpec(memory_space=pltpu.HBM)] * 4,
        out_specs=(vmem,) * (2 + len(state)),
        scratch_shapes=[
            pltpu.VMEM(queries.shape, queries.dtype),
            pltpu.SMEM(block_mask.shape, jnp.int32),
            pltpu.SemaphoreType.DMA((10 + 8 * side, ring // 2)),
            pltpu.SemaphoreType.DMA((2, devices)),
            pltpu.SemaphoreType.DMA((2,)),
            pltpu.SemaphoreType.DMA((2,)),
        ],
        compiler_params=pltpu.CompilerParams(
            collective_id=0, has_side_effects=True, vmem_limit_bytes=40 * 2**20
        ),
    )(in_hbm(queries), in_hbm(keys), in_hbm(values), in_hbm(block_mask))
    return True, ready, (all_keys, all_values)


def shards(queries, keys, values, block_mask):
    early, ready, everything = gathered(queries, keys, values, block_mask)
    vmem = pl.BlockSpec(memory_space=pltpu.VMEM)
    hbm = pl.BlockSpec(memory_space=pltpu.HBM)
    _, *sums = state_of(queries)
    parts = pl.cdiv(queries.shape[0], BLOCK)
    return pl.pallas_call(
        functools.partial(attend, early),
        out_shape=jax.ShapeDtypeStruct(queries.shape, jnp.float32),
        in_specs=[hbm] + [vmem] * 6,
        out_specs=hbm,
        scratch_shapes=[
            pltpu.SMEM(block_mask.shape, jnp.int32),
            pltpu.SMEM((parts, block_mask.shape[1]), jnp.int32),
            *[pltpu.VMEM(s.shape, s.dtype) for s in sums],
            pltpu.VMEM(queries.shape, jnp.float32),
            pltpu.SemaphoreType.DMA((parts,)),
            pltpu.SemaphoreType.DMA((1,)),
        ],
        compiler_params=pltpu.CompilerParams(vmem_limit_bytes=48 * 2**20),
    )(in_hbm(block_mask), *ready, *everything)


def solution(mesh):
    placed = (P(("qrow", "kcol"), None), P(("kcol", "qrow"), None), P(("kcol", "qrow"), None), P())
    return jax.shard_map(
        shards, mesh=mesh, in_specs=placed, out_specs=P(("qrow", "kcol"), None), check_vma=False
    )
```

```python
import functools
import math

import jax
import jax.numpy as jnp
from jax import lax
from jax.experimental import pallas as pl
from jax.experimental.pallas import tpu as pltpu
from jax.sharding import PartitionSpec as P

H = 4
DH = 128
BLOCK = 128
SIZES = (16, 8, 4)
NEAR = 3
TILE = 256
BIG = 4e30
MOST = 64
REACH = 1
HALVES = 1
SCAN = 16
NEG_FILL = -1e30
SCALE = math.log2(math.e) / math.sqrt(DH)


def columns_of(t):
    return slice(t * TILE, (t + 1) * TILE)


def prepare(q_ref, flipped, total, mass, top):
    tokens = q_ref.shape[0]
    part = min(tokens, BLOCK)
    width = H * part
    for own in range(tokens // part):
        turned = jnp.concatenate(
            [
                q_ref[own * part : (own + 1) * part, h * DH : (h + 1) * DH].T
                for h in range(H)
            ],
            axis=1,
        )
        scaled = turned.astype(jnp.float32) * SCALE
        coarse = scaled.astype(jnp.bfloat16)
        at = slice(own * width, (own + 1) * width)
        flipped[:DH, at] = coarse
        flipped[DH:, at] = (scaled - coarse.astype(jnp.float32)).astype(jnp.bfloat16)
    total[...] = jnp.zeros_like(total)
    mass[...] = jnp.zeros_like(mass)
    top[...] = jnp.full_like(top, NEG_FILL)


def operands(key_rows, value_rows):
    ones = jnp.ones((16, value_rows.shape[0]), jnp.bfloat16)
    return (
        jnp.concatenate([key_rows, key_rows], axis=1),
        jnp.concatenate([value_rows.T, ones], axis=0),
    )


def attend_to(state, lists, width, causal=None):
    flipped, total, mass, top = state
    tiles = flipped.shape[1] // TILE

    def scores_of(t):
        keys = lists[t * TILE // width][0]
        return jnp.dot(keys, flipped[:, columns_of(t)], preferred_element_type=jnp.float32)

    def weigh(t, scores):
        columns = columns_of(t)
        absent = lists[t * TILE // width][2]
        pieces = [scores[g * BLOCK : (g + 1) * BLOCK] for g in range(len(absent))]
        if causal is not None:
            pieces[0] = causal(t, pieces[0])
        old = top[:, columns]
        new = old
        for piece, off in zip(pieces, absent):
            new = jnp.maximum(new, jnp.max(piece, axis=0, keepdims=True) - off)
        top[:, columns] = new
        weights = [
            jnp.exp2(piece - (new + off)).astype(jnp.bfloat16)
            for piece, off in zip(pieces, absent)
        ]
        return jnp.exp2(old - new), jnp.concatenate(weights, axis=0)

    def gather(t, fade, weights):
        columns = columns_of(t)
        values = lists[t * TILE // width][1]
        summed = jnp.dot(values, weights, preferred_element_type=jnp.float32)
        mass[:, columns] = mass[:, columns] * fade + summed[DH : DH + 1]
        total[:, columns] = total[:, columns] * fade + summed[:DH]

    scores, held_back = scores_of(0), None
    for t in range(tiles):
        ahead = scores_of(t + 1) if t + 1 < tiles else None
        weighed = weigh(t, scores)
        if held_back is not None:
            gather(t - 1, *held_back)
        scores, held_back = ahead, weighed
    gather(tiles - 1, *held_back)


def penalty(here):
    return jnp.where(here, 0.0, BIG).astype(jnp.float32)


def absorbed(plane, q, z):
    spare = (plane < z) & (z + 1 < q)
    return (plane < q) & (plane - z <= REACH) & (z - plane <= REACH) & ~spare


def attend(
    early, mask_hbm, turned, old_total, old_mass, old_top, k_ref, v_ref, out_ref,
    mask_ref, listed, total, mass, top, held, sent, fetched,
):
    fetch = pltpu.make_async_copy(mask_hbm, mask_ref, fetched.at[0])
    fetch.start()
    tokens = out_ref.shape[0]
    part = min(tokens, BLOCK)
    pieces_here = tokens // part
    width = H * part
    last = mask_ref.shape[1] - 1
    q, c = lax.axis_index("qrow"), lax.axis_index("kcol")
    device = q * lax.axis_size("kcol") + c
    plane_blocks = 2 * lax.axis_size("qrow") * tokens // BLOCK
    firsts = [device * tokens + own * part for own in range(pieces_here)]
    rows = [first // BLOCK for first in firsts]
    state = (turned, total, mass, top)
    total[...] = old_total[...]
    mass[...] = old_mass[...]
    top[...] = old_top[...]

    def gone(block):
        if not early:
            return block < 0
        return absorbed(lax.div(block, plane_blocks), q, c // 2)

    def rows_of(ref, blocks):
        return jnp.concatenate(
            [ref[pl.ds(pl.multiple_of(b * BLOCK, BLOCK), BLOCK), :] for b in blocks], axis=0
        )

    def gathered_list(blocks, absent):
        keys, values = operands(rows_of(k_ref, blocks), rows_of(v_ref, blocks))
        return keys, values, absent

    def causal(t, piece):
        key_at = lax.broadcasted_iota(jnp.int32, piece.shape, 0)
        query_at = lax.broadcasted_iota(jnp.int32, piece.shape, 1) % part
        query_at = query_at + firsts[t * TILE // width] % BLOCK
        return jnp.where(key_at <= query_at, piece, -BIG)

    near = []
    for row in rows:
        blocks = [jnp.maximum(row - back, 0) for back in range(NEAR)]
        absent = [
            penalty((row >= back) & ~gone(block)) for back, block in enumerate(blocks)
        ]
        near.append(gathered_list(blocks, absent))
    attend_to(state, near, width, causal)

    fetch.wait()

    def scan(s, counts):
        lowest = last + 1 - (s + 1) * SCAN

        def note(_, counts):
            found = list(counts)
            for i in reversed(range(SCAN)):
                j = lowest + i
                for own, row in enumerate(rows):
                    listed[own, found[own]] = j
                    far = (j + NEAR <= row).astype(jnp.int32)
                    found[own] = found[own] + far * mask_ref[row, j]
            return tuple(found)

        skip = gone(lowest) | (lowest > rows[-1])
        return lax.fori_loop(0, jnp.where(skip, 0, 1), note, counts)

    counts = lax.fori_loop(
        0, (last + 1) // SCAN, scan, tuple(jnp.int32(0) for _ in rows)
    )
    most = counts[0]
    for count in counts[1:]:
        most = jnp.maximum(most, count)
    done = jnp.int32(0)
    for size in SIZES:
        left = most - done
        trips = left // size if size > SIZES[-1] else (left + size - 1) // size

        def step(t, carried, done=done, size=size):
            start = done + t * size
            lists = []
            for own, count in enumerate(counts):
                here = [start + g < count for g in range(size)]
                blocks = [
                    jnp.where(here[g], listed[own, jnp.minimum(start + g, last)], 0)
                    for g in range(size)
                ]
                lists.append(gathered_list(blocks, [penalty(ok) for ok in here]))
            attend_to(state, lists, width)
            return carried

        lax.fori_loop(0, trips, step, 0)
        done = done + trips * size

    copies = []
    for own in range(pieces_here):
        here = pl.ds(own * part, part)
        for h in range(H):
            at = slice(own * width + h * part, own * width + (h + 1) * part)
            held[here, h * DH : (h + 1) * DH] = (total[:, at] / mass[:, at]).T
        copy = pltpu.make_async_copy(held.at[here, :], out_ref.at[here, :], sent.at[own])
        copy.start()
        copies.append(copy)
    for copy in copies:
        copy.wait()


def spread(
    q_hbm, k_ref, v_ref, mask_hbm, k_all, v_all, flipped, total, mass, top,
    q_ref, mask_ref, send, recv, shared, local, fetched,
):
    ring, lane = lax.axis_size("kcol"), lax.axis_size("qrow")
    depth, width = ring // 2, lane // 2
    q, c = lax.axis_index("qrow"), lax.axis_index("kcol")
    level, core = c // 2, c % 2
    high, low = q // width, q % width
    tokens = k_ref.shape[0]
    own, whole = (k_ref, v_ref), (k_all, v_all)
    sibling = {"qrow": q, "kcol": level * 2 + (1 - core)}
    over = {"qrow": (1 - high) * width + low, "kcol": c}
    sides = [(low + i) % width for i in range(1, width)]
    beside = [{"qrow": high * width + i, "kcol": c} for i in sides]
    up = {"qrow": q, "kcol": c + 2}
    down = {"qrow": q, "kcol": c - 2}
    has_up, has_down = level < depth - 1, level > 0

    def slot(at, column, parity=core):
        return (at * 2 + parity) * lane + column

    def place(kv, block):
        return whole[kv].at[pl.ds(pl.multiple_of(block * tokens, tokens), tokens), :]

    copies = [
        pltpu.make_async_copy(own[kv], place(kv, slot(level, q)), local.at[kv]) for kv in range(2)
    ]
    for copy in copies:
        copy.start()

    fetches = [
        pltpu.make_async_copy(q_hbm, q_ref, fetched.at[0]),
        pltpu.make_async_copy(mask_hbm, mask_ref, fetched.at[1]),
    ]
    for fetch in fetches:
        fetch.start()

    barrier = pltpu.get_barrier_semaphore()

    def greet(target):
        pl.semaphore_signal(
            barrier, inc=1, device_id=target, device_id_type=pl.DeviceIdType.MESH
        )

    for target in [sibling, over] + beside:
        greet(target)
    pl.when(has_up)(lambda: greet(up))
    pl.when(has_down)(lambda: greet(down))
    ends = has_up.astype(jnp.int32) + has_down.astype(jnp.int32)
    pl.semaphore_wait(barrier, 2 + len(beside) + ends)

    for copy in copies:
        copy.wait()

    over_at, up_at, down_at = 1, 2, 2 + depth
    beside_at = 2 + 2 * depth
    relay_over_at = beside_at + len(beside)
    relay_beside_at = relay_over_at + 1

    def settled(semaphore, rows):
        span = k_all.at[pl.ds(0, rows), :]
        pltpu.make_async_copy(span, span, semaphore).wait()

    def landed(kv, block):
        settled(recv.at[kv, block], tokens)

    def push(kv, block, target, at, arrival=None):
        pltpu.make_async_remote_copy(
            src_ref=place(kv, block),
            dst_ref=place(kv, block),
            send_sem=send.at[at],
            recv_sem=recv.at[kv, block] if arrival is None else arrival,
            device_id=target,
            device_id_type=pl.DeviceIdType.MESH,
        ).start()

    def to_sibling(kv, block, at):
        push(kv, block, sibling, 0, shared.at[at])

    def guarded(ok, body):
        if ok is None:
            body()
        else:
            pl.when(ok)(body)

    def column_sends(ok, at, way):
        block = slot(at, q)

        def body():
            for kv in range(2):
                if way != 0:
                    landed(kv, block)
                if way >= 0:
                    pl.when(has_up)(lambda: push(kv, block, up, up_at + at))
                if way <= 0:
                    pl.when(has_down)(lambda: push(kv, block, down, down_at + at))
                push(kv, block, over, over_at)
                for i, target in enumerate(beside):
                    push(kv, block, target, beside_at + i)
                to_sibling(kv, block, at)

        guarded(ok, body)

    def relays(ok, at):
        def body():
            for i in sides:
                block = slot(at, high * width + i)
                landed(0, block)
                push(0, block, over, relay_over_at)
                to_sibling(0, block, at)
            block = slot(at, (1 - high) * width + low)
            for kv in (1, 0):
                landed(kv, block)
                if kv == 1:
                    for i, target in enumerate(beside):
                        push(1, block, target, relay_beside_at + i)
                to_sibling(kv, block, at)
            for i in sides:
                block = slot(at, high * width + i)
                landed(1, block)
                to_sibling(1, block, at)

        guarded(ok, body)

    def corners(ok, at):
        def body():
            for i in sides:
                block = slot(at, (1 - high) * width + i)
                for kv in range(2):
                    landed(kv, block)
                    to_sibling(kv, block, at)

        guarded(ok, body)

    def positions(step):
        if step == 0:
            return [(None, level, 0)]
        return [
            (level >= step, level - step, 1),
            (level + step < depth, level + step, -1),
        ]

    state = (flipped, total, mass, top)
    part = min(q_ref.shape[0], BLOCK)
    firsts = [(q * ring + c) * q_ref.shape[0] + own for own in range(0, q_ref.shape[0], part)]
    plane_tokens = 2 * lane * tokens
    half_tokens = plane_tokens // HALVES

    def absorb(step):
        for ok, at, _ in positions(step):
            here = absorbed(at, q, level) if ok is None else ok & absorbed(at, q, level)
            pl.when(here)(lambda at=at: settled(shared.at[at], plane_tokens))

        def half(i, carried):
            plane = jnp.where(i < HALVES, level - step, level + step)
            first = plane * plane_tokens + i % HALVES * half_tokens
            here = pl.ds(pl.multiple_of(first, half_tokens), half_tokens)
            keys, values = operands(k_all[here, :], v_all[here, :])
            lists = []
            for token in firsts:
                absent = [
                    (1 - mask_ref[token // BLOCK, first // BLOCK + g]).astype(jnp.float32) * BIG
                    for g in range(half_tokens // BLOCK)
                ]
                lists.append((keys, values, absent))
            attend_to(state, lists, H * part)
            return carried

        below = (level >= step) & absorbed(level - step, q, level)
        above = (level + step < depth) & (level + step < q) & (step > 0)
        lax.fori_loop(
            jnp.where(below, 0, HALVES), jnp.where(above, 2 * HALVES, HALVES), half, 0
        )

    for step in range(depth + 2):
        if step < depth:
            for ok, at, way in positions(step):
                column_sends(ok, at, way)
        if step == 0:
            for fetch in fetches:
                fetch.wait()
            prepare(q_ref, flipped, total, mass, top)
        if 1 <= step <= depth:
            for ok, at, _ in positions(step - 1):
                relays(ok, at)
        if step >= 2:
            for ok, at, _ in positions(step - 2):
                corners(ok, at)
            if step - 2 <= REACH:
                absorb(step - 2)
    for at in range(depth):
        pl.when(~absorbed(at, q, level))(lambda at=at: settled(shared.at[at], plane_tokens))
    settled(send.at[0], depth * plane_tokens)
    settled(send.at[over_at], 2 * depth * tokens)
    settled(send.at[relay_over_at], len(sides) * depth * tokens)
    for i in range(len(beside)):
        settled(send.at[beside_at + i], 2 * depth * tokens)
        settled(send.at[relay_beside_at + i], depth * tokens)
    for at in range(depth):
        pl.when(has_up & (level >= at))(lambda at=at: settled(send.at[up_at + at], 2 * tokens))
        pl.when(has_down & (level <= at))(
            lambda at=at: settled(send.at[down_at + at], 2 * tokens)
        )


def in_hbm(array):
    return pltpu.with_memory_space_constraint(array, pltpu.HBM)


def state_of(queries):
    columns = queries.shape[0] * H
    row = jax.ShapeDtypeStruct((1, columns), jnp.float32)
    return (
        jax.ShapeDtypeStruct((2 * DH, columns), jnp.bfloat16),
        jax.ShapeDtypeStruct((DH, columns), jnp.float32),
        row,
        row,
    )


def gathered(queries, keys, values, block_mask):
    ring, lane = lax.axis_size("kcol"), lax.axis_size("qrow")
    devices = ring * lane
    vmem = pl.BlockSpec(memory_space=pltpu.VMEM)
    state = state_of(queries)
    if ring != 2 * lane or lane % 2 or devices > MOST:
        both = ("kcol", "qrow")
        ready = pl.pallas_call(
            prepare, out_shape=state, in_specs=[vmem], out_specs=(vmem,) * len(state)
        )(queries)
        return False, ready, (
            lax.all_gather(keys, both, axis=0, tiled=True),
            lax.all_gather(values, both, axis=0, tiled=True),
        )
    full = jax.ShapeDtypeStruct((keys.shape[0] * devices, keys.shape[1]), keys.dtype)
    side = lane // 2 - 1
    all_keys, all_values, *ready = pl.pallas_call(
        spread,
        out_shape=(full, full) + state,
        in_specs=[pl.BlockSpec(memory_space=pltpu.HBM)] * 4,
        out_specs=(vmem,) * (2 + len(state)),
        scratch_shapes=[
            pltpu.VMEM(queries.shape, queries.dtype),
            pltpu.SMEM(block_mask.shape, jnp.int32),
            pltpu.SemaphoreType.DMA((3 + ring + 2 * side,)),
            pltpu.SemaphoreType.DMA((2, devices)),
            pltpu.SemaphoreType.DMA((ring // 2,)),
            pltpu.SemaphoreType.DMA((2,)),
            pltpu.SemaphoreType.DMA((2,)),
        ],
        compiler_params=pltpu.CompilerParams(
            collective_id=0, has_side_effects=True, vmem_limit_bytes=40 * 2**20
        ),
    )(in_hbm(queries), in_hbm(keys), in_hbm(values), in_hbm(block_mask))
    return True, ready, (all_keys, all_values)


def shards(queries, keys, values, block_mask):
    early, ready, everything = gathered(queries, keys, values, block_mask)
    vmem = pl.BlockSpec(memory_space=pltpu.VMEM)
    hbm = pl.BlockSpec(memory_space=pltpu.HBM)
    _, *sums = state_of(queries)
    parts = pl.cdiv(queries.shape[0], BLOCK)
    return pl.pallas_call(
        functools.partial(attend, early),
        out_shape=jax.ShapeDtypeStruct(queries.shape, jnp.float32),
        in_specs=[hbm] + [vmem] * 6,
        out_specs=hbm,
        scratch_shapes=[
            pltpu.SMEM(block_mask.shape, jnp.int32),
            pltpu.SMEM((parts, block_mask.shape[1]), jnp.int32),
            *[pltpu.VMEM(s.shape, s.dtype) for s in sums],
            pltpu.VMEM(queries.shape, jnp.float32),
            pltpu.SemaphoreType.DMA((parts,)),
            pltpu.SemaphoreType.DMA((1,)),
        ],
        compiler_params=pltpu.CompilerParams(vmem_limit_bytes=48 * 2**20),
    )(in_hbm(block_mask), *ready, *everything)


def solution(mesh):
    placed = (P(("qrow", "kcol"), None), P(("kcol", "qrow"), None), P(("kcol", "qrow"), None), P())
    return jax.shard_map(
        shards, mesh=mesh, in_specs=placed, out_specs=P(("qrow", "kcol"), None), check_vma=False
    )
```

```python
import functools
import math

import jax
import jax.numpy as jnp
from jax import lax
from jax.experimental import pallas as pl
from jax.experimental.pallas import tpu as pltpu
from jax.sharding import PartitionSpec as P

H = 4
DH = 128
BLOCK = 128
SIZES = (16, 8, 4)
NEAR = 3
TILE = 256
BIG = 4e30
MOST = 64
REACH = 1
HALVES = 1
SCAN = 16
NEG_FILL = -1e30
SCALE = math.log2(math.e) / math.sqrt(DH)


def columns_of(t):
    return slice(t * TILE, (t + 1) * TILE)


def prepare(q_ref, flipped, total, mass, top):
    tokens = q_ref.shape[0]
    part = min(tokens, BLOCK)
    width = H * part
    for own in range(tokens // part):
        turned = jnp.concatenate(
            [
                q_ref[own * part : (own + 1) * part, h * DH : (h + 1) * DH].T
                for h in range(H)
            ],
            axis=1,
        )
        scaled = turned.astype(jnp.float32) * SCALE
        coarse = scaled.astype(jnp.bfloat16)
        at = slice(own * width, (own + 1) * width)
        flipped[:DH, at] = coarse
        flipped[DH:, at] = (scaled - coarse.astype(jnp.float32)).astype(jnp.bfloat16)
    total[...] = jnp.zeros_like(total)
    mass[...] = jnp.zeros_like(mass)
    top[...] = jnp.full_like(top, NEG_FILL)


def operands(key_rows, value_rows):
    ones = jnp.ones((16, value_rows.shape[0]), jnp.bfloat16)
    return (
        jnp.concatenate([key_rows, key_rows], axis=1),
        jnp.concatenate([value_rows.T, ones], axis=0),
    )


def attend_to(state, lists, width, causal=None):
    flipped, total, mass, top = state
    tiles = flipped.shape[1] // TILE

    def scores_of(t):
        keys = lists[t * TILE // width][0]
        return jnp.dot(keys, flipped[:, columns_of(t)], preferred_element_type=jnp.float32)

    def weigh(t, scores):
        columns = columns_of(t)
        absent = lists[t * TILE // width][2]
        pieces = [scores[g * BLOCK : (g + 1) * BLOCK] for g in range(len(absent))]
        if causal is not None:
            pieces[0] = causal(t, pieces[0])
        old = top[:, columns]
        new = old
        for piece, off in zip(pieces, absent):
            new = jnp.maximum(new, jnp.max(piece, axis=0, keepdims=True) - off)
        top[:, columns] = new
        weights = [
            jnp.exp2(piece - (new + off)).astype(jnp.bfloat16)
            for piece, off in zip(pieces, absent)
        ]
        return jnp.exp2(old - new), jnp.concatenate(weights, axis=0)

    def gather(t, fade, weights):
        columns = columns_of(t)
        values = lists[t * TILE // width][1]
        summed = jnp.dot(values, weights, preferred_element_type=jnp.float32)
        mass[:, columns] = mass[:, columns] * fade + summed[DH : DH + 1]
        total[:, columns] = total[:, columns] * fade + summed[:DH]

    scores, held_back = scores_of(0), None
    for t in range(tiles):
        ahead = scores_of(t + 1) if t + 1 < tiles else None
        weighed = weigh(t, scores)
        if held_back is not None:
            gather(t - 1, *held_back)
        scores, held_back = ahead, weighed
    gather(tiles - 1, *held_back)


def penalty(here):
    return jnp.where(here, 0.0, BIG).astype(jnp.float32)


def absorbed(plane, q, z):
    spare = (plane < z) & (z + 1 < q)
    return (plane < q) & (plane - z <= REACH) & (z - plane <= REACH) & ~spare


def attend(
    early, mask_hbm, turned, old_total, old_mass, old_top, k_ref, v_ref, out_ref,
    mask_ref, listed, total, mass, top, held, sent, fetched,
):
    fetch = pltpu.make_async_copy(mask_hbm, mask_ref, fetched.at[0])
    fetch.start()
    tokens = out_ref.shape[0]
    part = min(tokens, BLOCK)
    pieces_here = tokens // part
    width = H * part
    last = mask_ref.shape[1] - 1
    q, c = lax.axis_index("qrow"), lax.axis_index("kcol")
    device = q * lax.axis_size("kcol") + c
    plane_blocks = 2 * lax.axis_size("qrow") * tokens // BLOCK
    firsts = [device * tokens + own * part for own in range(pieces_here)]
    rows = [first // BLOCK for first in firsts]
    state = (turned, total, mass, top)
    total[...] = old_total[...]
    mass[...] = old_mass[...]
    top[...] = old_top[...]

    def gone(block):
        if not early:
            return block < 0
        return absorbed(lax.div(block, plane_blocks), q, c // 2)

    def rows_of(ref, blocks):
        return jnp.concatenate(
            [ref[pl.ds(pl.multiple_of(b * BLOCK, BLOCK), BLOCK), :] for b in blocks], axis=0
        )

    def gathered_list(blocks, absent):
        keys, values = operands(rows_of(k_ref, blocks), rows_of(v_ref, blocks))
        return keys, values, absent

    def causal(t, piece):
        key_at = lax.broadcasted_iota(jnp.int32, piece.shape, 0)
        query_at = lax.broadcasted_iota(jnp.int32, piece.shape, 1) % part
        query_at = query_at + firsts[t * TILE // width] % BLOCK
        return jnp.where(key_at <= query_at, piece, -BIG)

    near = []
    for row in rows:
        blocks = [jnp.maximum(row - back, 0) for back in range(NEAR)]
        absent = [
            penalty((row >= back) & ~gone(block)) for back, block in enumerate(blocks)
        ]
        near.append(gathered_list(blocks, absent))
    attend_to(state, near, width, causal)

    fetch.wait()

    def scan(s, counts):
        lowest = last + 1 - (s + 1) * SCAN

        def note(_, counts):
            found = list(counts)
            for i in reversed(range(SCAN)):
                j = lowest + i
                for own, row in enumerate(rows):
                    listed[own, found[own]] = j
                    far = (j + NEAR <= row).astype(jnp.int32)
                    found[own] = found[own] + far * mask_ref[row, j]
            return tuple(found)

        skip = gone(lowest) | (lowest > rows[-1])
        return lax.fori_loop(0, jnp.where(skip, 0, 1), note, counts)

    counts = lax.fori_loop(
        0, (last + 1) // SCAN, scan, tuple(jnp.int32(0) for _ in rows)
    )
    most = counts[0]
    for count in counts[1:]:
        most = jnp.maximum(most, count)
    done = jnp.int32(0)
    for size in SIZES:
        left = most - done
        trips = left // size if size > SIZES[-1] else (left + size - 1) // size

        def step(t, carried, done=done, size=size):
            start = done + t * size
            lists = []
            for own, count in enumerate(counts):
                here = [start + g < count for g in range(size)]
                blocks = [
                    jnp.where(here[g], listed[own, jnp.minimum(start + g, last)], 0)
                    for g in range(size)
                ]
                lists.append(gathered_list(blocks, [penalty(ok) for ok in here]))
            attend_to(state, lists, width)
            return carried

        lax.fori_loop(0, trips, step, 0)
        done = done + trips * size

    copies = []
    for own in range(pieces_here):
        here = pl.ds(own * part, part)
        for h in range(H):
            at = slice(own * width + h * part, own * width + (h + 1) * part)
            held[here, h * DH : (h + 1) * DH] = (total[:, at] / mass[:, at]).T
        copy = pltpu.make_async_copy(held.at[here, :], out_ref.at[here, :], sent.at[own])
        copy.start()
        copies.append(copy)
    for copy in copies:
        copy.wait()


def spread(
    q_hbm, k_ref, v_ref, mask_hbm, k_all, v_all, flipped, total, mass, top,
    q_ref, mask_ref, send, recv, shared, local, fetched,
):
    ring, lane = lax.axis_size("kcol"), lax.axis_size("qrow")
    depth, width = ring // 2, lane // 2
    q, c = lax.axis_index("qrow"), lax.axis_index("kcol")
    level, core = c // 2, c % 2
    high, low = q // width, q % width
    tokens = k_ref.shape[0]
    own, whole = (k_ref, v_ref), (k_all, v_all)
    sibling = {"qrow": q, "kcol": level * 2 + (1 - core)}
    over = {"qrow": (1 - high) * width + low, "kcol": c}
    sides = [(low + i) % width for i in range(1, width)]
    beside = [{"qrow": high * width + i, "kcol": c} for i in sides]
    up = {"qrow": q, "kcol": c + 2}
    down = {"qrow": q, "kcol": c - 2}
    has_up, has_down = level < depth - 1, level > 0

    def slot(at, column, parity=core):
        return (at * 2 + parity) * lane + column

    def place(kv, block):
        return whole[kv].at[pl.ds(pl.multiple_of(block * tokens, tokens), tokens), :]

    copies = [
        pltpu.make_async_copy(own[kv], place(kv, slot(level, q)), local.at[kv]) for kv in range(2)
    ]
    for copy in copies:
        copy.start()

    fetches = [
        pltpu.make_async_copy(q_hbm, q_ref, fetched.at[0]),
        pltpu.make_async_copy(mask_hbm, mask_ref, fetched.at[1]),
    ]
    for fetch in fetches:
        fetch.start()

    barrier = pltpu.get_barrier_semaphore()

    def greet(target):
        pl.semaphore_signal(
            barrier, inc=1, device_id=target, device_id_type=pl.DeviceIdType.MESH
        )

    for target in [sibling, over] + beside:
        greet(target)
    pl.when(has_up)(lambda: greet(up))
    pl.when(has_down)(lambda: greet(down))
    ends = has_up.astype(jnp.int32) + has_down.astype(jnp.int32)
    pl.semaphore_wait(barrier, 2 + len(beside) + ends)

    for copy in copies:
        copy.wait()

    over_at, up_at, down_at = 1, 2, 2 + depth
    beside_at = 2 + 2 * depth
    relay_over_at = beside_at + len(beside)
    relay_beside_at = relay_over_at + 1
    lift_at = relay_beside_at + len(beside)
    spare_at = lift_at + 2

    def settled(semaphore, rows):
        span = k_all.at[pl.ds(0, rows), :]
        pltpu.make_async_copy(span, span, semaphore).wait()

    def landed(kv, block):
        settled(recv.at[kv, block], tokens)

    def push(kv, block, target, at, arrival=None):
        pltpu.make_async_remote_copy(
            src_ref=place(kv, block),
            dst_ref=place(kv, block),
            send_sem=send.at[at],
            recv_sem=recv.at[kv, block] if arrival is None else arrival,
            device_id=target,
            device_id_type=pl.DeviceIdType.MESH,
        ).start()

    def to_sibling(kv, block, at):
        push(kv, block, sibling, 0, shared.at[at])

    def guarded(ok, body):
        if ok is None:
            body()
        else:
            pl.when(ok)(body)

    def lifted(at):
        return ((at == 0) & (level >= 2)) | ((at == depth - 1) & (level < depth - 2))

    def across_levels(relayed, at, body):
        if relayed:
            body()
        else:
            pl.when(~lifted(at))(body)

    def lift(kv, block, at, way):
        if way > 0:
            pl.when((at == 0) & has_up)(lambda: push(kv, block, up, lift_at))
        if way < 0:
            pl.when((at == depth - 1) & has_down)(lambda: push(kv, block, down, lift_at + 1))

    def column_sends(ok, at, way):
        block = slot(at, q)

        def body():
            for kv in range(2):
                if way != 0:
                    landed(kv, block)
                if way >= 0:
                    pl.when(has_up)(lambda: push(kv, block, up, up_at + at))
                if way <= 0:
                    pl.when(has_down)(lambda: push(kv, block, down, down_at + at))
                relayed = kv == 1 or way == 0
                across_levels(relayed, at, lambda: push(kv, block, over, over_at if relayed else spare_at + at))
                relayed = kv == 0 or way == 0

                def spread_out():
                    for i, target in enumerate(beside):
                        push(kv, block, target, beside_at + i if relayed else spare_at + at)

                across_levels(relayed, at, spread_out)
                to_sibling(kv, block, at)

        guarded(ok, body)

    def relays(ok, at, way):
        def body():
            for i in sides:
                block = slot(at, high * width + i)
                landed(0, block)
                push(0, block, over, relay_over_at)
                to_sibling(0, block, at)
            block = slot(at, (1 - high) * width + low)
            for kv in (1, 0):
                landed(kv, block)
                if kv == 1:
                    for i, target in enumerate(beside):
                        push(1, block, target, relay_beside_at + i)
                else:
                    lift(0, block, at, way)
                to_sibling(kv, block, at)
            for i in sides:
                block = slot(at, high * width + i)
                landed(1, block)
                lift(1, block, at, way)
                to_sibling(1, block, at)

        guarded(ok, body)

    def corners(ok, at):
        def body():
            for i in sides:
                block = slot(at, (1 - high) * width + i)
                for kv in range(2):
                    landed(kv, block)
                    to_sibling(kv, block, at)

        guarded(ok, body)

    def positions(step):
        if step == 0:
            return [(None, level, 0)]
        return [
            (level >= step, level - step, 1),
            (level + step < depth, level + step, -1),
        ]

    state = (flipped, total, mass, top)
    part = min(q_ref.shape[0], BLOCK)
    firsts = [(q * ring + c) * q_ref.shape[0] + own for own in range(0, q_ref.shape[0], part)]
    plane_tokens = 2 * lane * tokens
    half_tokens = plane_tokens // HALVES

    def absorb(step):
        for ok, at, _ in positions(step):
            here = absorbed(at, q, level) if ok is None else ok & absorbed(at, q, level)
            pl.when(here)(lambda at=at: settled(shared.at[at], plane_tokens))

        def half(i, carried):
            plane = jnp.where(i < HALVES, level - step, level + step)
            first = plane * plane_tokens + i % HALVES * half_tokens
            here = pl.ds(pl.multiple_of(first, half_tokens), half_tokens)
            keys, values = operands(k_all[here, :], v_all[here, :])
            lists = []
            for token in firsts:
                absent = [
                    (1 - mask_ref[token // BLOCK, first // BLOCK + g]).astype(jnp.float32) * BIG
                    for g in range(half_tokens // BLOCK)
                ]
                lists.append((keys, values, absent))
            attend_to(state, lists, H * part)
            return carried

        below = (level >= step) & absorbed(level - step, q, level)
        above = (level + step < depth) & (level + step < q) & (step > 0)
        lax.fori_loop(
            jnp.where(below, 0, HALVES), jnp.where(above, 2 * HALVES, HALVES), half, 0
        )

    for step in range(depth + 2):
        if step < depth:
            for ok, at, way in positions(step):
                column_sends(ok, at, way)
        if step == 0:
            for fetch in fetches:
                fetch.wait()
            prepare(q_ref, flipped, total, mass, top)
        if 1 <= step <= depth:
            for ok, at, way in positions(step - 1):
                relays(ok, at, way)
        if step >= 2:
            for ok, at, _ in positions(step - 2):
                corners(ok, at)
            if step - 2 <= REACH:
                absorb(step - 2)
    for at in range(depth):
        pl.when(~absorbed(at, q, level))(lambda at=at: settled(shared.at[at], plane_tokens))
    settled(send.at[0], depth * plane_tokens)
    settled(send.at[over_at], (depth + 1) * tokens)
    settled(send.at[relay_over_at], len(sides) * depth * tokens)
    for i in range(len(beside)):
        settled(send.at[beside_at + i], (depth + 1) * tokens)
        settled(send.at[relay_beside_at + i], depth * tokens)
    pl.when(has_up & (level > 0))(
        lambda: settled(send.at[lift_at], (len(sides) + 1) * tokens)
    )
    pl.when(has_down & (level < depth - 1))(
        lambda: settled(send.at[lift_at + 1], (len(sides) + 1) * tokens)
    )
    for at in range(depth):
        pl.when((level != at) & ~lifted(at))(
            lambda at=at: settled(send.at[spare_at + at], (1 + len(beside)) * tokens)
        )
    for at in range(depth):
        pl.when(has_up & (level >= at))(lambda at=at: settled(send.at[up_at + at], 2 * tokens))
        pl.when(has_down & (level <= at))(
            lambda at=at: settled(send.at[down_at + at], 2 * tokens)
        )


def in_hbm(array):
    return pltpu.with_memory_space_constraint(array, pltpu.HBM)


def state_of(queries):
    columns = queries.shape[0] * H
    row = jax.ShapeDtypeStruct((1, columns), jnp.float32)
    return (
        jax.ShapeDtypeStruct((2 * DH, columns), jnp.bfloat16),
        jax.ShapeDtypeStruct((DH, columns), jnp.float32),
        row,
        row,
    )


def gathered(queries, keys, values, block_mask):
    ring, lane = lax.axis_size("kcol"), lax.axis_size("qrow")
    devices = ring * lane
    vmem = pl.BlockSpec(memory_space=pltpu.VMEM)
    state = state_of(queries)
    if ring != 2 * lane or lane % 2 or devices > MOST:
        both = ("kcol", "qrow")
        ready = pl.pallas_call(
            prepare, out_shape=state, in_specs=[vmem], out_specs=(vmem,) * len(state)
        )(queries)
        return False, ready, (
            lax.all_gather(keys, both, axis=0, tiled=True),
            lax.all_gather(values, both, axis=0, tiled=True),
        )
    full = jax.ShapeDtypeStruct((keys.shape[0] * devices, keys.shape[1]), keys.dtype)
    side = lane // 2 - 1
    all_keys, all_values, *ready = pl.pallas_call(
        spread,
        out_shape=(full, full) + state,
        in_specs=[pl.BlockSpec(memory_space=pltpu.HBM)] * 4,
        out_specs=(vmem,) * (2 + len(state)),
        scratch_shapes=[
            pltpu.VMEM(queries.shape, queries.dtype),
            pltpu.SMEM(block_mask.shape, jnp.int32),
            pltpu.SemaphoreType.DMA((5 + ring + ring // 2 + 2 * side,)),
            pltpu.SemaphoreType.DMA((2, devices)),
            pltpu.SemaphoreType.DMA((ring // 2,)),
            pltpu.SemaphoreType.DMA((2,)),
            pltpu.SemaphoreType.DMA((2,)),
        ],
        compiler_params=pltpu.CompilerParams(
            collective_id=0, has_side_effects=True, vmem_limit_bytes=40 * 2**20
        ),
    )(in_hbm(queries), in_hbm(keys), in_hbm(values), in_hbm(block_mask))
    return True, ready, (all_keys, all_values)


def shards(queries, keys, values, block_mask):
    early, ready, everything = gathered(queries, keys, values, block_mask)
    vmem = pl.BlockSpec(memory_space=pltpu.VMEM)
    hbm = pl.BlockSpec(memory_space=pltpu.HBM)
    _, *sums = state_of(queries)
    parts = pl.cdiv(queries.shape[0], BLOCK)
    return pl.pallas_call(
        functools.partial(attend, early),
        out_shape=jax.ShapeDtypeStruct(queries.shape, jnp.float32),
        in_specs=[hbm] + [vmem] * 6,
        out_specs=hbm,
        scratch_shapes=[
            pltpu.SMEM(block_mask.shape, jnp.int32),
            pltpu.SMEM((parts, block_mask.shape[1]), jnp.int32),
            *[pltpu.VMEM(s.shape, s.dtype) for s in sums],
            pltpu.VMEM(queries.shape, jnp.float32),
            pltpu.SemaphoreType.DMA((parts,)),
            pltpu.SemaphoreType.DMA((1,)),
        ],
        compiler_params=pltpu.CompilerParams(vmem_limit_bytes=48 * 2**20),
    )(in_hbm(block_mask), *ready, *everything)


def solution(mesh):
    placed = (P(("qrow", "kcol"), None), P(("kcol", "qrow"), None), P(("kcol", "qrow"), None), P())
    return jax.shard_map(
        shards, mesh=mesh, in_specs=placed, out_specs=P(("qrow", "kcol"), None), check_vma=False
    )
```

```python
import functools
import math

import jax
import jax.numpy as jnp
from jax import lax
from jax.experimental import pallas as pl
from jax.experimental.pallas import tpu as pltpu
from jax.sharding import PartitionSpec as P

H = 4
DH = 128
BLOCK = 128
SIZES = (16, 8, 4)
NEAR = 3
TILE = 256
BIG = 4e30
MOST = 64
REACH = 1
HALVES = 1
SCAN = 16
NEG_FILL = -1e30
SCALE = math.log2(math.e) / math.sqrt(DH)


def columns_of(t):
    return slice(t * TILE, (t + 1) * TILE)


def prepare(q_ref, flipped, total, mass, top):
    tokens = q_ref.shape[0]
    part = min(tokens, BLOCK)
    width = H * part
    for own in range(tokens // part):
        turned = jnp.concatenate(
            [
                q_ref[own * part : (own + 1) * part, h * DH : (h + 1) * DH].T
                for h in range(H)
            ],
            axis=1,
        )
        scaled = turned.astype(jnp.float32) * SCALE
        coarse = scaled.astype(jnp.bfloat16)
        at = slice(own * width, (own + 1) * width)
        flipped[:DH, at] = coarse
        flipped[DH:, at] = (scaled - coarse.astype(jnp.float32)).astype(jnp.bfloat16)
    total[...] = jnp.zeros_like(total)
    mass[...] = jnp.zeros_like(mass)
    top[...] = jnp.full_like(top, NEG_FILL)


def operands(key_rows, value_rows):
    ones = jnp.ones((16, value_rows.shape[0]), jnp.bfloat16)
    return (
        jnp.concatenate([key_rows, key_rows], axis=1),
        jnp.concatenate([value_rows.T, ones], axis=0),
    )


def attend_to(state, lists, width, causal=None):
    flipped, total, mass, top = state
    tiles = flipped.shape[1] // TILE

    def scores_of(t):
        keys = lists[t * TILE // width][0]
        return jnp.dot(keys, flipped[:, columns_of(t)], preferred_element_type=jnp.float32)

    def weigh(t, scores):
        columns = columns_of(t)
        absent = lists[t * TILE // width][2]
        pieces = [scores[g * BLOCK : (g + 1) * BLOCK] for g in range(len(absent))]
        if causal is not None:
            pieces[0] = causal(t, pieces[0])
        old = top[:, columns]
        new = old
        for piece, off in zip(pieces, absent):
            new = jnp.maximum(new, jnp.max(piece, axis=0, keepdims=True) - off)
        top[:, columns] = new
        weights = [
            jnp.exp2(piece - (new + off)).astype(jnp.bfloat16)
            for piece, off in zip(pieces, absent)
        ]
        return jnp.exp2(old - new), jnp.concatenate(weights, axis=0)

    def gather(t, fade, weights):
        columns = columns_of(t)
        values = lists[t * TILE // width][1]
        summed = jnp.dot(values, weights, preferred_element_type=jnp.float32)
        mass[:, columns] = mass[:, columns] * fade + summed[DH : DH + 1]
        total[:, columns] = total[:, columns] * fade + summed[:DH]

    scores, held_back = scores_of(0), None
    for t in range(tiles):
        ahead = scores_of(t + 1) if t + 1 < tiles else None
        weighed = weigh(t, scores)
        if held_back is not None:
            gather(t - 1, *held_back)
        scores, held_back = ahead, weighed
    gather(tiles - 1, *held_back)


def penalty(here):
    return jnp.where(here, 0.0, BIG).astype(jnp.float32)


def absorbed(plane, q, z):
    spare = (plane < z) & (z + 1 < q)
    return (plane < q) & (plane - z <= REACH) & (z - plane <= REACH) & ~spare


def attend(
    early, mask_hbm, turned, old_total, old_mass, old_top, k_ref, v_ref, out_ref,
    mask_ref, listed, total, mass, top, held, sent, fetched,
):
    fetch = pltpu.make_async_copy(mask_hbm, mask_ref, fetched.at[0])
    fetch.start()
    tokens = out_ref.shape[0]
    part = min(tokens, BLOCK)
    pieces_here = tokens // part
    width = H * part
    last = mask_ref.shape[1] - 1
    q, c = lax.axis_index("qrow"), lax.axis_index("kcol")
    device = q * lax.axis_size("kcol") + c
    plane_blocks = 2 * lax.axis_size("qrow") * tokens // BLOCK
    firsts = [device * tokens + own * part for own in range(pieces_here)]
    rows = [first // BLOCK for first in firsts]
    state = (turned, total, mass, top)
    total[...] = old_total[...]
    mass[...] = old_mass[...]
    top[...] = old_top[...]

    def gone(block):
        if not early:
            return block < 0
        return absorbed(lax.div(block, plane_blocks), q, c // 2)

    def rows_of(ref, blocks):
        return jnp.concatenate(
            [ref[pl.ds(pl.multiple_of(b * BLOCK, BLOCK), BLOCK), :] for b in blocks], axis=0
        )

    def gathered_list(blocks, absent):
        keys, values = operands(rows_of(k_ref, blocks), rows_of(v_ref, blocks))
        return keys, values, absent

    def causal(t, piece):
        key_at = lax.broadcasted_iota(jnp.int32, piece.shape, 0)
        query_at = lax.broadcasted_iota(jnp.int32, piece.shape, 1) % part
        query_at = query_at + firsts[t * TILE // width] % BLOCK
        return jnp.where(key_at <= query_at, piece, -BIG)

    near = []
    for row in rows:
        blocks = [jnp.maximum(row - back, 0) for back in range(NEAR)]
        absent = [
            penalty((row >= back) & ~gone(block)) for back, block in enumerate(blocks)
        ]
        near.append(gathered_list(blocks, absent))
    attend_to(state, near, width, causal)

    fetch.wait()

    def scan(s, counts):
        lowest = last + 1 - (s + 1) * SCAN

        def note(_, counts):
            found = list(counts)
            for i in reversed(range(SCAN)):
                j = lowest + i
                for own, row in enumerate(rows):
                    listed[own, found[own]] = j
                    far = (j + NEAR <= row).astype(jnp.int32)
                    found[own] = found[own] + far * mask_ref[row, j]
            return tuple(found)

        skip = gone(lowest) | (lowest > rows[-1])
        return lax.fori_loop(0, jnp.where(skip, 0, 1), note, counts)

    counts = lax.fori_loop(
        0, (last + 1) // SCAN, scan, tuple(jnp.int32(0) for _ in rows)
    )
    most = counts[0]
    for count in counts[1:]:
        most = jnp.maximum(most, count)
    done = jnp.int32(0)
    for size in SIZES:
        left = most - done
        trips = left // size if size > SIZES[-1] else (left + size - 1) // size

        def step(t, carried, done=done, size=size):
            start = done + t * size
            lists = []
            for own, count in enumerate(counts):
                here = [start + g < count for g in range(size)]
                blocks = [
                    jnp.where(here[g], listed[own, jnp.minimum(start + g, last)], 0)
                    for g in range(size)
                ]
                lists.append(gathered_list(blocks, [penalty(ok) for ok in here]))
            attend_to(state, lists, width)
            return carried

        lax.fori_loop(0, trips, step, 0)
        done = done + trips * size

    copies = []
    for own in range(pieces_here):
        here = pl.ds(own * part, part)
        for h in range(H):
            at = slice(own * width + h * part, own * width + (h + 1) * part)
            held[here, h * DH : (h + 1) * DH] = (total[:, at] / mass[:, at]).T
        copy = pltpu.make_async_copy(held.at[here, :], out_ref.at[here, :], sent.at[own])
        copy.start()
        copies.append(copy)
    for copy in copies:
        copy.wait()


def spread(
    q_hbm, k_ref, v_ref, mask_hbm, k_all, v_all, flipped, total, mass, top,
    q_ref, mask_ref, send, recv, shared, local, fetched,
):
    ring, lane = lax.axis_size("kcol"), lax.axis_size("qrow")
    depth, width = ring // 2, lane // 2
    q, c = lax.axis_index("qrow"), lax.axis_index("kcol")
    level, core = c // 2, c % 2
    high, low = q // width, q % width
    tokens = k_ref.shape[0]
    own, whole = (k_ref, v_ref), (k_all, v_all)
    sibling = {"qrow": q, "kcol": level * 2 + (1 - core)}
    over = {"qrow": (1 - high) * width + low, "kcol": c}
    sides = [(low + i) % width for i in range(1, width)]
    beside = [{"qrow": high * width + i, "kcol": c} for i in sides]
    up = {"qrow": q, "kcol": c + 2}
    down = {"qrow": q, "kcol": c - 2}
    has_up, has_down = level < depth - 1, level > 0

    def slot(at, column, parity=core):
        return (at * 2 + parity) * lane + column

    def place(kv, block):
        return whole[kv].at[pl.ds(pl.multiple_of(block * tokens, tokens), tokens), :]

    copies = [
        pltpu.make_async_copy(own[kv], place(kv, slot(level, q)), local.at[kv]) for kv in range(2)
    ]
    for copy in copies:
        copy.start()

    fetches = [
        pltpu.make_async_copy(q_hbm, q_ref, fetched.at[0]),
        pltpu.make_async_copy(mask_hbm, mask_ref, fetched.at[1]),
    ]
    for fetch in fetches:
        fetch.start()

    barrier = pltpu.get_barrier_semaphore()

    def greet(target):
        pl.semaphore_signal(
            barrier, inc=1, device_id=target, device_id_type=pl.DeviceIdType.MESH
        )

    for target in [sibling, over] + beside:
        greet(target)
    pl.when(has_up)(lambda: greet(up))
    pl.when(has_down)(lambda: greet(down))
    ends = has_up.astype(jnp.int32) + has_down.astype(jnp.int32)
    pl.semaphore_wait(barrier, 2 + len(beside) + ends)

    for copy in copies:
        copy.wait()

    final = depth - 1
    mine = q == lane - 1
    over_last = (high == 0) & (low == width - 1)
    over_at, up_at, down_at = 1, 2, 2 + depth
    beside_at = 2 + 2 * depth
    relay_over_at = beside_at + len(beside)
    relay_beside_at = relay_over_at + 1
    lift_at = relay_beside_at + len(beside)
    spare_at = lift_at + 2
    end_over_at = spare_at + depth
    end_beside_at = end_over_at + 2
    end_relay_over_at = end_beside_at + 2 * len(beside)
    end_relay_beside_at = end_relay_over_at + 1

    def beside_last(i):
        return high * width + i == lane - 1

    def end_over(kv):
        return high == 0 if kv == 1 else over_last

    def end_beside(kv, i):
        return i == width - 1 if kv == 0 else beside_last(i)

    def settled(semaphore, rows):
        span = k_all.at[pl.ds(0, rows), :]
        pltpu.make_async_copy(span, span, semaphore).wait()

    def landed(kv, block):
        settled(recv.at[kv, block], tokens)

    def push(kv, block, target, at, arrival=None):
        pltpu.make_async_remote_copy(
            src_ref=place(kv, block),
            dst_ref=place(kv, block),
            send_sem=send.at[at],
            recv_sem=recv.at[kv, block] if arrival is None else arrival,
            device_id=target,
            device_id_type=pl.DeviceIdType.MESH,
        ).start()

    def to_sibling(kv, block, at):
        push(kv, block, sibling, 0, shared.at[at])

    def guarded(ok, body):
        if ok is None:
            body()
        else:
            pl.when(ok)(body)

    def lifted(at):
        return ((at == 0) & (level >= 2)) | ((at == depth - 1) & (level < depth - 2))

    def sent_where(at, way, conditions, body):
        if way <= 0:
            conditions = conditions[:1] + [(at != final) | conditions[1]]
        else:
            conditions = conditions[:1]
        conditions = [c for c in conditions if c is not None]
        if not conditions:
            body()
        else:
            ok = conditions[0]
            for c in conditions[1:]:
                ok &= c
            pl.when(ok)(body)

    def either(at, way, end, usual):
        return jnp.where(at == final, end, usual) if way <= 0 else usual

    def lift(kv, block, at, way):
        if way > 0:
            pl.when((at == 0) & has_up)(lambda: push(kv, block, up, lift_at))
        if way < 0:
            pl.when((at == depth - 1) & has_down)(lambda: push(kv, block, down, lift_at + 1))

    def column_sends(ok, at, way):
        block = slot(at, q)

        def body():
            for kv in range(2):
                if way != 0:
                    landed(kv, block)
                if way >= 0:
                    pl.when(has_up)(lambda: push(kv, block, up, up_at + at))
                if way <= 0:
                    pl.when(has_down)(lambda: push(kv, block, down, down_at + at))
                on_time = None if kv == 1 or way == 0 else ~lifted(at)
                usual = over_at if kv == 1 else spare_at + at
                sent_where(
                    at, way, [on_time, end_over(kv)],
                    lambda: push(kv, block, over, either(at, way, end_over_at + kv, usual)),
                )
                on_time = None if kv == 0 or way == 0 else ~lifted(at)
                for i, (column, target) in enumerate(zip(sides, beside)):
                    usual = beside_at + i if kv == 0 else spare_at + at
                    sent_where(
                        at, way, [on_time, end_beside(kv, column)],
                        lambda: push(
                            kv, block, target,
                            either(at, way, end_beside_at + 2 * i + kv, usual),
                        ),
                    )
                sent_where(at, way, [None, mine], lambda: to_sibling(kv, block, at))

        guarded(ok, body)

    def relays(ok, at, way):
        def body():
            def keys_over():
                for i in sides:
                    block = slot(at, high * width + i)
                    landed(0, block)
                    at_end = end_relay_over_at
                    sent_where(
                        at, way, [None, over_last],
                        lambda: push(0, block, over, either(at, way, at_end, relay_over_at)),
                    )
                    sent_where(at, way, [None, mine], lambda: to_sibling(0, block, at))

            def values_beside():
                block = slot(at, (1 - high) * width + low)
                landed(1, block)
                for i, (column, target) in enumerate(zip(sides, beside)):
                    at_end = end_relay_beside_at + i
                    sent_where(
                        at, way, [None, beside_last(column)],
                        lambda: push(
                            1, block, target, either(at, way, at_end, relay_beside_at + i)
                        ),
                    )
                sent_where(at, way, [None, mine], lambda: to_sibling(1, block, at))

            def rest():
                block = slot(at, (1 - high) * width + low)
                landed(0, block)
                lift(0, block, at, way)
                to_sibling(0, block, at)
                for i in sides:
                    block = slot(at, high * width + i)
                    landed(1, block)
                    lift(1, block, at, way)
                    to_sibling(1, block, at)

            sent_where(at, way, [None, low == width - 1], keys_over)
            sent_where(at, way, [None, high == 1], values_beside)
            sent_where(at, way, [None, mine], rest)

        guarded(ok, body)

    def corners(ok, at, way):
        def body():
            for i in sides:
                block = slot(at, (1 - high) * width + i)
                for kv in range(2):
                    landed(kv, block)
                    to_sibling(kv, block, at)

        if way <= 0:
            needed = (at != final) | mine
            ok = needed if ok is None else ok & needed
        guarded(ok, body)

    def positions(step):
        if step == 0:
            return [(None, level, 0)]
        return [
            (level >= step, level - step, 1),
            (level + step < depth, level + step, -1),
        ]

    state = (flipped, total, mass, top)
    part = min(q_ref.shape[0], BLOCK)
    firsts = [(q * ring + c) * q_ref.shape[0] + own for own in range(0, q_ref.shape[0], part)]
    plane_tokens = 2 * lane * tokens
    half_tokens = plane_tokens // HALVES

    def absorb(step):
        for ok, at, _ in positions(step):
            here = absorbed(at, q, level) if ok is None else ok & absorbed(at, q, level)
            pl.when(here)(lambda at=at: settled(shared.at[at], plane_tokens))

        def half(i, carried):
            plane = jnp.where(i < HALVES, level - step, level + step)
            first = plane * plane_tokens + i % HALVES * half_tokens
            here = pl.ds(pl.multiple_of(first, half_tokens), half_tokens)
            keys, values = operands(k_all[here, :], v_all[here, :])
            lists = []
            for token in firsts:
                absent = [
                    (1 - mask_ref[token // BLOCK, first // BLOCK + g]).astype(jnp.float32) * BIG
                    for g in range(half_tokens // BLOCK)
                ]
                lists.append((keys, values, absent))
            attend_to(state, lists, H * part)
            return carried

        below = (level >= step) & absorbed(level - step, q, level)
        above = (level + step < depth) & (level + step < q) & (step > 0)
        lax.fori_loop(
            jnp.where(below, 0, HALVES), jnp.where(above, 2 * HALVES, HALVES), half, 0
        )

    for step in range(depth + 2):
        if step < depth:
            for ok, at, way in positions(step):
                column_sends(ok, at, way)
        if step == 0:
            for fetch in fetches:
                fetch.wait()
            prepare(q_ref, flipped, total, mass, top)
        if 1 <= step <= depth:
            for ok, at, way in positions(step - 1):
                relays(ok, at, way)
        if step >= 2:
            for ok, at, way in positions(step - 2):
                corners(ok, at, way)
            if step - 2 <= REACH:
                absorb(step - 2)
    for at in range(depth):
        here = ~absorbed(at, q, level)
        if at == final:
            here &= mine
        pl.when(here)(lambda at=at: settled(shared.at[at], plane_tokens))
    pl.when(mine)(lambda: settled(send.at[0], depth * plane_tokens))
    pl.when(~mine)(lambda: settled(send.at[0], final * plane_tokens))
    settled(send.at[over_at], final * tokens)
    settled(send.at[relay_over_at], len(sides) * final * tokens)
    pl.when(over_last)(lambda: settled(send.at[end_relay_over_at], len(sides) * tokens))
    for i, column in enumerate(sides):
        settled(send.at[beside_at + i], final * tokens)
        settled(send.at[relay_beside_at + i], final * tokens)
        pl.when(beside_last(column))(
            lambda i=i: settled(send.at[end_relay_beside_at + i], tokens)
        )
    for kv in range(2):
        on_time = ~lifted(final)
        late = end_over(kv) & on_time if kv == 0 else end_over(kv)
        pl.when(late)(lambda kv=kv: settled(send.at[end_over_at + kv], tokens))
        for i, column in enumerate(sides):
            late = end_beside(kv, column) & on_time if kv == 1 else end_beside(kv, column)
            pl.when(late)(
                lambda i=i, kv=kv: settled(send.at[end_beside_at + 2 * i + kv], tokens)
            )
    lifts = (len(sides) + 1) * tokens
    pl.when(has_up & (level > 0))(lambda: settled(send.at[lift_at], lifts))
    pl.when(has_down & (level < final) & mine)(
        lambda: settled(send.at[lift_at + 1], lifts)
    )
    for at in range(final):
        pl.when(~lifted(at))(
            lambda at=at: settled(send.at[spare_at + at], (1 + len(beside)) * tokens)
        )
    for at in range(depth):
        pl.when(has_up & (level >= at))(lambda at=at: settled(send.at[up_at + at], 2 * tokens))
        pl.when(has_down & (level <= at))(
            lambda at=at: settled(send.at[down_at + at], 2 * tokens)
        )


def in_hbm(array):
    return pltpu.with_memory_space_constraint(array, pltpu.HBM)


def state_of(queries):
    columns = queries.shape[0] * H
    row = jax.ShapeDtypeStruct((1, columns), jnp.float32)
    return (
        jax.ShapeDtypeStruct((2 * DH, columns), jnp.bfloat16),
        jax.ShapeDtypeStruct((DH, columns), jnp.float32),
        row,
        row,
    )


def gathered(queries, keys, values, block_mask):
    ring, lane = lax.axis_size("kcol"), lax.axis_size("qrow")
    devices = ring * lane
    vmem = pl.BlockSpec(memory_space=pltpu.VMEM)
    state = state_of(queries)
    if ring != 2 * lane or lane % 2 or devices > MOST:
        both = ("kcol", "qrow")
        ready = pl.pallas_call(
            prepare, out_shape=state, in_specs=[vmem], out_specs=(vmem,) * len(state)
        )(queries)
        return False, ready, (
            lax.all_gather(keys, both, axis=0, tiled=True),
            lax.all_gather(values, both, axis=0, tiled=True),
        )
    full = jax.ShapeDtypeStruct((keys.shape[0] * devices, keys.shape[1]), keys.dtype)
    side = lane // 2 - 1
    all_keys, all_values, *ready = pl.pallas_call(
        spread,
        out_shape=(full, full) + state,
        in_specs=[pl.BlockSpec(memory_space=pltpu.HBM)] * 4,
        out_specs=(vmem,) * (2 + len(state)),
        scratch_shapes=[
            pltpu.VMEM(queries.shape, queries.dtype),
            pltpu.SMEM(block_mask.shape, jnp.int32),
            pltpu.SemaphoreType.DMA((8 + ring + ring // 2 + 5 * side,)),
            pltpu.SemaphoreType.DMA((2, devices)),
            pltpu.SemaphoreType.DMA((ring // 2,)),
            pltpu.SemaphoreType.DMA((2,)),
            pltpu.SemaphoreType.DMA((2,)),
        ],
        compiler_params=pltpu.CompilerParams(
            collective_id=0, has_side_effects=True, vmem_limit_bytes=40 * 2**20
        ),
    )(in_hbm(queries), in_hbm(keys), in_hbm(values), in_hbm(block_mask))
    return True, ready, (all_keys, all_values)


def shards(queries, keys, values, block_mask):
    early, ready, everything = gathered(queries, keys, values, block_mask)
    vmem = pl.BlockSpec(memory_space=pltpu.VMEM)
    hbm = pl.BlockSpec(memory_space=pltpu.HBM)
    _, *sums = state_of(queries)
    parts = pl.cdiv(queries.shape[0], BLOCK)
    return pl.pallas_call(
        functools.partial(attend, early),
        out_shape=jax.ShapeDtypeStruct(queries.shape, jnp.float32),
        in_specs=[hbm] + [vmem] * 6,
        out_specs=hbm,
        scratch_shapes=[
            pltpu.SMEM(block_mask.shape, jnp.int32),
            pltpu.SMEM((parts, block_mask.shape[1]), jnp.int32),
            *[pltpu.VMEM(s.shape, s.dtype) for s in sums],
            pltpu.VMEM(queries.shape, jnp.float32),
            pltpu.SemaphoreType.DMA((parts,)),
            pltpu.SemaphoreType.DMA((1,)),
        ],
        compiler_params=pltpu.CompilerParams(vmem_limit_bytes=48 * 2**20),
    )(in_hbm(block_mask), *ready, *everything)


def solution(mesh):
    placed = (P(("qrow", "kcol"), None), P(("kcol", "qrow"), None), P(("kcol", "qrow"), None), P())
    return jax.shard_map(
        shards, mesh=mesh, in_specs=placed, out_specs=P(("qrow", "kcol"), None), check_vma=False
    )
```

```python
import functools
import math

import jax
import jax.numpy as jnp
from jax import lax
from jax.experimental import pallas as pl
from jax.experimental.pallas import tpu as pltpu
from jax.sharding import PartitionSpec as P

H = 4
DH = 128
BLOCK = 128
SIZES = (20, 12, 4)
NEAR = 3
TILE = 256
BIG = 4e30
MOST = 64
REACH = 1
HALVES = 1
SCAN = 16
NEG_FILL = -1e30
SCALE = math.log2(math.e) / math.sqrt(DH)


def columns_of(t):
    return slice(t * TILE, (t + 1) * TILE)


def prepare(q_ref, flipped, total, mass, top):
    tokens = q_ref.shape[0]
    part = min(tokens, BLOCK)
    width = H * part
    for own in range(tokens // part):
        turned = jnp.concatenate(
            [
                q_ref[own * part : (own + 1) * part, h * DH : (h + 1) * DH].T
                for h in range(H)
            ],
            axis=1,
        )
        scaled = turned.astype(jnp.float32) * SCALE
        coarse = scaled.astype(jnp.bfloat16)
        at = slice(own * width, (own + 1) * width)
        flipped[:DH, at] = coarse
        flipped[DH:, at] = (scaled - coarse.astype(jnp.float32)).astype(jnp.bfloat16)
    total[...] = jnp.zeros_like(total)
    mass[...] = jnp.zeros_like(mass)
    top[...] = jnp.full_like(top, NEG_FILL)


def operands(key_rows, value_rows):
    ones = jnp.ones((16, value_rows.shape[0]), jnp.bfloat16)
    return (
        jnp.concatenate([key_rows, key_rows], axis=1),
        jnp.concatenate([value_rows.T, ones], axis=0),
    )


def attend_to(state, lists, width, causal=None):
    flipped, total, mass, top = state
    tiles = flipped.shape[1] // TILE

    def scores_of(t):
        keys = lists[t * TILE // width][0]
        return jnp.dot(keys, flipped[:, columns_of(t)], preferred_element_type=jnp.float32)

    def weigh(t, scores):
        columns = columns_of(t)
        absent = lists[t * TILE // width][2]
        pieces = [scores[g * BLOCK : (g + 1) * BLOCK] for g in range(len(absent))]
        if causal is not None:
            pieces[0] = causal(t, pieces[0])
        old = top[:, columns]
        new = old
        for piece, off in zip(pieces, absent):
            new = jnp.maximum(new, jnp.max(piece, axis=0, keepdims=True) - off)
        top[:, columns] = new
        weights = [
            jnp.exp2(piece - (new + off)).astype(jnp.bfloat16)
            for piece, off in zip(pieces, absent)
        ]
        return jnp.exp2(old - new), jnp.concatenate(weights, axis=0)

    def gather(t, fade, weights):
        columns = columns_of(t)
        values = lists[t * TILE // width][1]
        summed = jnp.dot(values, weights, preferred_element_type=jnp.float32)
        mass[:, columns] = mass[:, columns] * fade + summed[DH : DH + 1]
        total[:, columns] = total[:, columns] * fade + summed[:DH]

    scores, held_back = scores_of(0), None
    for t in range(tiles):
        ahead = scores_of(t + 1) if t + 1 < tiles else None
        weighed = weigh(t, scores)
        if held_back is not None:
            gather(t - 1, *held_back)
        scores, held_back = ahead, weighed
    gather(tiles - 1, *held_back)


def penalty(here):
    return jnp.where(here, 0.0, BIG).astype(jnp.float32)


def absorbed(plane, q, z):
    spare = (plane < z) & (z + 1 < q)
    return (plane < q) & (plane - z <= REACH) & (z - plane <= REACH) & ~spare


def attend(
    early, mask_hbm, turned, old_total, old_mass, old_top, k_ref, v_ref, out_ref,
    mask_ref, listed, total, mass, top, held, sent, fetched,
):
    fetch = pltpu.make_async_copy(mask_hbm, mask_ref, fetched.at[0])
    fetch.start()
    tokens = out_ref.shape[0]
    part = min(tokens, BLOCK)
    pieces_here = tokens // part
    width = H * part
    last = mask_ref.shape[1] - 1
    q, c = lax.axis_index("qrow"), lax.axis_index("kcol")
    device = q * lax.axis_size("kcol") + c
    plane_blocks = 2 * lax.axis_size("qrow") * tokens // BLOCK
    firsts = [device * tokens + own * part for own in range(pieces_here)]
    rows = [first // BLOCK for first in firsts]
    state = (turned, total, mass, top)
    total[...] = old_total[...]
    mass[...] = old_mass[...]
    top[...] = old_top[...]

    def gone(block):
        if not early:
            return block < 0
        return absorbed(lax.div(block, plane_blocks), q, c // 2)

    def rows_of(ref, blocks):
        return jnp.concatenate(
            [ref[pl.ds(pl.multiple_of(b * BLOCK, BLOCK), BLOCK), :] for b in blocks], axis=0
        )

    def gathered_list(blocks, absent):
        keys, values = operands(rows_of(k_ref, blocks), rows_of(v_ref, blocks))
        return keys, values, absent

    def causal(t, piece):
        key_at = lax.broadcasted_iota(jnp.int32, piece.shape, 0)
        query_at = lax.broadcasted_iota(jnp.int32, piece.shape, 1) % part
        query_at = query_at + firsts[t * TILE // width] % BLOCK
        return jnp.where(key_at <= query_at, piece, -BIG)

    near = []
    for row in rows:
        blocks = [jnp.maximum(row - back, 0) for back in range(NEAR)]
        absent = [
            penalty((row >= back) & ~gone(block)) for back, block in enumerate(blocks)
        ]
        near.append(gathered_list(blocks, absent))
    attend_to(state, near, width, causal)

    fetch.wait()

    def scan(s, counts):
        lowest = last + 1 - (s + 1) * SCAN

        def note(_, counts):
            found = list(counts)
            for i in reversed(range(SCAN)):
                j = lowest + i
                for own, row in enumerate(rows):
                    listed[own, found[own]] = j
                    far = (j + NEAR <= row).astype(jnp.int32)
                    found[own] = found[own] + far * mask_ref[row, j]
            return tuple(found)

        skip = gone(lowest) | (lowest > rows[-1])
        return lax.fori_loop(0, jnp.where(skip, 0, 1), note, counts)

    counts = lax.fori_loop(
        0, (last + 1) // SCAN, scan, tuple(jnp.int32(0) for _ in rows)
    )
    most = counts[0]
    for count in counts[1:]:
        most = jnp.maximum(most, count)
    done = jnp.int32(0)
    for size, smaller in zip(SIZES, SIZES[1:] + (0,)):
        left = most - done
        trips = jnp.where(left > smaller, (left + size - smaller - 1) // size, 0)

        def step(t, carried, done=done, size=size):
            start = done + t * size
            lists = []
            for own, count in enumerate(counts):
                here = [start + g < count for g in range(size)]
                blocks = [
                    jnp.where(here[g], listed[own, jnp.minimum(start + g, last)], 0)
                    for g in range(size)
                ]
                lists.append(gathered_list(blocks, [penalty(ok) for ok in here]))
            attend_to(state, lists, width)
            return carried

        lax.fori_loop(0, trips, step, 0)
        done = done + trips * size

    copies = []
    for own in range(pieces_here):
        here = pl.ds(own * part, part)
        for h in range(H):
            at = slice(own * width + h * part, own * width + (h + 1) * part)
            held[here, h * DH : (h + 1) * DH] = (total[:, at] / mass[:, at]).T
        copy = pltpu.make_async_copy(held.at[here, :], out_ref.at[here, :], sent.at[own])
        copy.start()
        copies.append(copy)
    for copy in copies:
        copy.wait()


def spread(
    q_hbm, k_ref, v_ref, mask_hbm, k_all, v_all, flipped, total, mass, top,
    q_ref, mask_ref, send, recv, shared, local, fetched,
):
    ring, lane = lax.axis_size("kcol"), lax.axis_size("qrow")
    depth, width = ring // 2, lane // 2
    q, c = lax.axis_index("qrow"), lax.axis_index("kcol")
    level, core = c // 2, c % 2
    high, low = q // width, q % width
    tokens = k_ref.shape[0]
    own, whole = (k_ref, v_ref), (k_all, v_all)
    sibling = {"qrow": q, "kcol": level * 2 + (1 - core)}
    over = {"qrow": (1 - high) * width + low, "kcol": c}
    sides = [(low + i) % width for i in range(1, width)]
    beside = [{"qrow": high * width + i, "kcol": c} for i in sides]
    up = {"qrow": q, "kcol": c + 2}
    down = {"qrow": q, "kcol": c - 2}
    has_up, has_down = level < depth - 1, level > 0

    def slot(at, column, parity=core):
        return (at * 2 + parity) * lane + column

    def place(kv, block):
        return whole[kv].at[pl.ds(pl.multiple_of(block * tokens, tokens), tokens), :]

    copies = [
        pltpu.make_async_copy(own[kv], place(kv, slot(level, q)), local.at[kv]) for kv in range(2)
    ]
    for copy in copies:
        copy.start()

    fetches = [
        pltpu.make_async_copy(q_hbm, q_ref, fetched.at[0]),
        pltpu.make_async_copy(mask_hbm, mask_ref, fetched.at[1]),
    ]
    for fetch in fetches:
        fetch.start()

    barrier = pltpu.get_barrier_semaphore()

    def greet(target):
        pl.semaphore_signal(
            barrier, inc=1, device_id=target, device_id_type=pl.DeviceIdType.MESH
        )

    for target in [sibling, over] + beside:
        greet(target)
    pl.when(has_up)(lambda: greet(up))
    pl.when(has_down)(lambda: greet(down))
    ends = has_up.astype(jnp.int32) + has_down.astype(jnp.int32)
    pl.semaphore_wait(barrier, 2 + len(beside) + ends)

    for copy in copies:
        copy.wait()

    final = depth - 1
    mine = q == lane - 1
    over_last = (high == 0) & (low == width - 1)
    over_at, up_at, down_at = 1, 2, 2 + depth
    beside_at = 2 + 2 * depth
    relay_over_at = beside_at + len(beside)
    relay_beside_at = relay_over_at + 1
    lift_at = relay_beside_at + len(beside)
    spare_at = lift_at + 2
    end_over_at = spare_at + depth
    end_beside_at = end_over_at + 2
    end_relay_over_at = end_beside_at + 2 * len(beside)
    end_relay_beside_at = end_relay_over_at + 1

    def beside_last(i):
        return high * width + i == lane - 1

    def end_over(kv):
        return high == 0 if kv == 1 else over_last

    def end_beside(kv, i):
        return i == width - 1 if kv == 0 else beside_last(i)

    def settled(semaphore, rows):
        span = k_all.at[pl.ds(0, rows), :]
        pltpu.make_async_copy(span, span, semaphore).wait()

    def landed(kv, block):
        settled(recv.at[kv, block], tokens)

    def push(kv, block, target, at, arrival=None):
        pltpu.make_async_remote_copy(
            src_ref=place(kv, block),
            dst_ref=place(kv, block),
            send_sem=send.at[at],
            recv_sem=recv.at[kv, block] if arrival is None else arrival,
            device_id=target,
            device_id_type=pl.DeviceIdType.MESH,
        ).start()

    def to_sibling(kv, block, at):
        push(kv, block, sibling, 0, shared.at[at])

    def guarded(ok, body):
        if ok is None:
            body()
        else:
            pl.when(ok)(body)

    def lifted(at):
        return ((at == 0) & (level >= 2)) | ((at == depth - 1) & (level < depth - 2))

    def sent_where(at, way, conditions, body):
        if way <= 0:
            conditions = conditions[:1] + [(at != final) | conditions[1]]
        else:
            conditions = conditions[:1]
        conditions = [c for c in conditions if c is not None]
        if not conditions:
            body()
        else:
            ok = conditions[0]
            for c in conditions[1:]:
                ok &= c
            pl.when(ok)(body)

    def either(at, way, end, usual):
        return jnp.where(at == final, end, usual) if way <= 0 else usual

    def lift(kv, block, at, way):
        if way > 0:
            pl.when((at == 0) & has_up)(lambda: push(kv, block, up, lift_at))
        if way < 0:
            pl.when((at == depth - 1) & has_down)(lambda: push(kv, block, down, lift_at + 1))

    def column_sends(ok, at, way):
        block = slot(at, q)

        def body():
            for kv in range(2):
                if way != 0:
                    landed(kv, block)
                if way >= 0:
                    pl.when(has_up)(lambda: push(kv, block, up, up_at + at))
                if way <= 0:
                    pl.when(has_down)(lambda: push(kv, block, down, down_at + at))
                on_time = None if kv == 1 or way == 0 else ~lifted(at)
                usual = over_at if kv == 1 else spare_at + at
                sent_where(
                    at, way, [on_time, end_over(kv)],
                    lambda: push(kv, block, over, either(at, way, end_over_at + kv, usual)),
                )
                on_time = None if kv == 0 or way == 0 else ~lifted(at)
                for i, (column, target) in enumerate(zip(sides, beside)):
                    usual = beside_at + i if kv == 0 else spare_at + at
                    sent_where(
                        at, way, [on_time, end_beside(kv, column)],
                        lambda: push(
                            kv, block, target,
                            either(at, way, end_beside_at + 2 * i + kv, usual),
                        ),
                    )
                sent_where(at, way, [None, mine], lambda: to_sibling(kv, block, at))

        guarded(ok, body)

    def relays(ok, at, way):
        def body():
            def keys_over():
                for i in sides:
                    block = slot(at, high * width + i)
                    landed(0, block)
                    at_end = end_relay_over_at
                    sent_where(
                        at, way, [None, over_last],
                        lambda: push(0, block, over, either(at, way, at_end, relay_over_at)),
                    )
                    sent_where(at, way, [None, mine], lambda: to_sibling(0, block, at))

            def values_beside():
                block = slot(at, (1 - high) * width + low)
                landed(1, block)
                for i, (column, target) in enumerate(zip(sides, beside)):
                    at_end = end_relay_beside_at + i
                    sent_where(
                        at, way, [None, beside_last(column)],
                        lambda: push(
                            1, block, target, either(at, way, at_end, relay_beside_at + i)
                        ),
                    )
                sent_where(at, way, [None, mine], lambda: to_sibling(1, block, at))

            def rest():
                block = slot(at, (1 - high) * width + low)
                landed(0, block)
                lift(0, block, at, way)
                to_sibling(0, block, at)
                for i in sides:
                    block = slot(at, high * width + i)
                    landed(1, block)
                    lift(1, block, at, way)
                    to_sibling(1, block, at)

            sent_where(at, way, [None, low == width - 1], keys_over)
            sent_where(at, way, [None, high == 1], values_beside)
            sent_where(at, way, [None, mine], rest)

        guarded(ok, body)

    def corners(ok, at, way):
        def body():
            for i in sides:
                block = slot(at, (1 - high) * width + i)
                for kv in range(2):
                    landed(kv, block)
                    to_sibling(kv, block, at)

        if way <= 0:
            needed = (at != final) | mine
            ok = needed if ok is None else ok & needed
        guarded(ok, body)

    def positions(step):
        if step == 0:
            return [(None, level, 0)]
        return [
            (level >= step, level - step, 1),
            (level + step < depth, level + step, -1),
        ]

    state = (flipped, total, mass, top)
    part = min(q_ref.shape[0], BLOCK)
    firsts = [(q * ring + c) * q_ref.shape[0] + own for own in range(0, q_ref.shape[0], part)]
    plane_tokens = 2 * lane * tokens
    half_tokens = plane_tokens // HALVES

    def absorb(step):
        for ok, at, _ in positions(step):
            here = absorbed(at, q, level) if ok is None else ok & absorbed(at, q, level)
            pl.when(here)(lambda at=at: settled(shared.at[at], plane_tokens))

        def half(i, carried):
            plane = jnp.where(i < HALVES, level - step, level + step)
            first = plane * plane_tokens + i % HALVES * half_tokens
            here = pl.ds(pl.multiple_of(first, half_tokens), half_tokens)
            keys, values = operands(k_all[here, :], v_all[here, :])
            lists = []
            for token in firsts:
                absent = [
                    (1 - mask_ref[token // BLOCK, first // BLOCK + g]).astype(jnp.float32) * BIG
                    for g in range(half_tokens // BLOCK)
                ]
                lists.append((keys, values, absent))
            attend_to(state, lists, H * part)
            return carried

        below = (level >= step) & absorbed(level - step, q, level)
        above = (level + step < depth) & (level + step < q) & (step > 0)
        lax.fori_loop(
            jnp.where(below, 0, HALVES), jnp.where(above, 2 * HALVES, HALVES), half, 0
        )

    for step in range(depth + 2):
        if step < depth:
            for ok, at, way in positions(step):
                column_sends(ok, at, way)
        if step == 0:
            for fetch in fetches:
                fetch.wait()
            prepare(q_ref, flipped, total, mass, top)
        if 1 <= step <= depth:
            for ok, at, way in positions(step - 1):
                relays(ok, at, way)
        if step >= 2:
            for ok, at, way in positions(step - 2):
                corners(ok, at, way)
            if step - 2 <= REACH:
                absorb(step - 2)
    for at in range(depth):
        here = ~absorbed(at, q, level)
        if at == final:
            here &= mine
        pl.when(here)(lambda at=at: settled(shared.at[at], plane_tokens))
    pl.when(mine)(lambda: settled(send.at[0], depth * plane_tokens))
    pl.when(~mine)(lambda: settled(send.at[0], final * plane_tokens))
    settled(send.at[over_at], final * tokens)
    settled(send.at[relay_over_at], len(sides) * final * tokens)
    pl.when(over_last)(lambda: settled(send.at[end_relay_over_at], len(sides) * tokens))
    for i, column in enumerate(sides):
        settled(send.at[beside_at + i], final * tokens)
        settled(send.at[relay_beside_at + i], final * tokens)
        pl.when(beside_last(column))(
            lambda i=i: settled(send.at[end_relay_beside_at + i], tokens)
        )
    for kv in range(2):
        on_time = ~lifted(final)
        late = end_over(kv) & on_time if kv == 0 else end_over(kv)
        pl.when(late)(lambda kv=kv: settled(send.at[end_over_at + kv], tokens))
        for i, column in enumerate(sides):
            late = end_beside(kv, column) & on_time if kv == 1 else end_beside(kv, column)
            pl.when(late)(
                lambda i=i, kv=kv: settled(send.at[end_beside_at + 2 * i + kv], tokens)
            )
    lifts = (len(sides) + 1) * tokens
    pl.when(has_up & (level > 0))(lambda: settled(send.at[lift_at], lifts))
    pl.when(has_down & (level < final) & mine)(
        lambda: settled(send.at[lift_at + 1], lifts)
    )
    for at in range(final):
        pl.when(~lifted(at))(
            lambda at=at: settled(send.at[spare_at + at], (1 + len(beside)) * tokens)
        )
    for at in range(depth):
        pl.when(has_up & (level >= at))(lambda at=at: settled(send.at[up_at + at], 2 * tokens))
        pl.when(has_down & (level <= at))(
            lambda at=at: settled(send.at[down_at + at], 2 * tokens)
        )


def in_hbm(array):
    return pltpu.with_memory_space_constraint(array, pltpu.HBM)


def state_of(queries):
    columns = queries.shape[0] * H
    row = jax.ShapeDtypeStruct((1, columns), jnp.float32)
    return (
        jax.ShapeDtypeStruct((2 * DH, columns), jnp.bfloat16),
        jax.ShapeDtypeStruct((DH, columns), jnp.float32),
        row,
        row,
    )


def gathered(queries, keys, values, block_mask):
    ring, lane = lax.axis_size("kcol"), lax.axis_size("qrow")
    devices = ring * lane
    vmem = pl.BlockSpec(memory_space=pltpu.VMEM)
    state = state_of(queries)
    if ring != 2 * lane or lane % 2 or devices > MOST:
        both = ("kcol", "qrow")
        ready = pl.pallas_call(
            prepare, out_shape=state, in_specs=[vmem], out_specs=(vmem,) * len(state)
        )(queries)
        return False, ready, (
            lax.all_gather(keys, both, axis=0, tiled=True),
            lax.all_gather(values, both, axis=0, tiled=True),
        )
    full = jax.ShapeDtypeStruct((keys.shape[0] * devices, keys.shape[1]), keys.dtype)
    side = lane // 2 - 1
    all_keys, all_values, *ready = pl.pallas_call(
        spread,
        out_shape=(full, full) + state,
        in_specs=[pl.BlockSpec(memory_space=pltpu.HBM)] * 4,
        out_specs=(vmem,) * (2 + len(state)),
        scratch_shapes=[
            pltpu.VMEM(queries.shape, queries.dtype),
            pltpu.SMEM(block_mask.shape, jnp.int32),
            pltpu.SemaphoreType.DMA((8 + ring + ring // 2 + 5 * side,)),
            pltpu.SemaphoreType.DMA((2, devices)),
            pltpu.SemaphoreType.DMA((ring // 2,)),
            pltpu.SemaphoreType.DMA((2,)),
            pltpu.SemaphoreType.DMA((2,)),
        ],
        compiler_params=pltpu.CompilerParams(
            collective_id=0, has_side_effects=True, vmem_limit_bytes=40 * 2**20
        ),
    )(in_hbm(queries), in_hbm(keys), in_hbm(values), in_hbm(block_mask))
    return True, ready, (all_keys, all_values)


def shards(queries, keys, values, block_mask):
    early, ready, everything = gathered(queries, keys, values, block_mask)
    vmem = pl.BlockSpec(memory_space=pltpu.VMEM)
    hbm = pl.BlockSpec(memory_space=pltpu.HBM)
    _, *sums = state_of(queries)
    parts = pl.cdiv(queries.shape[0], BLOCK)
    return pl.pallas_call(
        functools.partial(attend, early),
        out_shape=jax.ShapeDtypeStruct(queries.shape, jnp.float32),
        in_specs=[hbm] + [vmem] * 6,
        out_specs=hbm,
        scratch_shapes=[
            pltpu.SMEM(block_mask.shape, jnp.int32),
            pltpu.SMEM((parts, block_mask.shape[1]), jnp.int32),
            *[pltpu.VMEM(s.shape, s.dtype) for s in sums],
            pltpu.VMEM(queries.shape, jnp.float32),
            pltpu.SemaphoreType.DMA((parts,)),
            pltpu.SemaphoreType.DMA((1,)),
        ],
        compiler_params=pltpu.CompilerParams(vmem_limit_bytes=48 * 2**20),
    )(in_hbm(block_mask), *ready, *everything)


def solution(mesh):
    placed = (P(("qrow", "kcol"), None), P(("kcol", "qrow"), None), P(("kcol", "qrow"), None), P())
    return jax.shard_map(
        shards, mesh=mesh, in_specs=placed, out_specs=P(("qrow", "kcol"), None), check_vma=False
    )
```

```python
import functools
import math

import jax
import jax.numpy as jnp
from jax import lax
from jax.experimental import pallas as pl
from jax.experimental.pallas import tpu as pltpu
from jax.sharding import PartitionSpec as P

H = 4
DH = 128
BLOCK = 128
SIZES = (20, 12, 4)
NEAR = 3
TILE = 256
BIG = 4e30
MOST = 64
REACH = 1
HALVES = 1
SCAN = 16
NEG_FILL = -1e30
SCALE = math.log2(math.e) / math.sqrt(DH)


def columns_of(t):
    return slice(t * TILE, (t + 1) * TILE)


def prepare(q_ref, flipped, total, mass, top):
    tokens = q_ref.shape[0]
    part = min(tokens, BLOCK)
    width = H * part
    for own in range(tokens // part):
        turned = jnp.concatenate(
            [
                q_ref[own * part : (own + 1) * part, h * DH : (h + 1) * DH].T
                for h in range(H)
            ],
            axis=1,
        )
        scaled = turned.astype(jnp.float32) * SCALE
        coarse = scaled.astype(jnp.bfloat16)
        at = slice(own * width, (own + 1) * width)
        flipped[:DH, at] = coarse
        flipped[DH:, at] = (scaled - coarse.astype(jnp.float32)).astype(jnp.bfloat16)
    total[...] = jnp.zeros_like(total)
    mass[...] = jnp.zeros_like(mass)
    top[...] = jnp.full_like(top, NEG_FILL)


def operands(key_rows, value_rows):
    ones = jnp.ones((16, value_rows.shape[0]), jnp.bfloat16)
    return (
        jnp.concatenate([key_rows, key_rows], axis=1),
        jnp.concatenate([value_rows.T, ones], axis=0),
    )


def attend_to(state, lists, width, causal=None):
    flipped, total, mass, top = state
    tiles = flipped.shape[1] // TILE

    def scores_of(t):
        keys = lists[t * TILE // width][0]
        return jnp.dot(keys, flipped[:, columns_of(t)], preferred_element_type=jnp.float32)

    def weigh(t, scores):
        columns = columns_of(t)
        absent = lists[t * TILE // width][2]
        pieces = [scores[g * BLOCK : (g + 1) * BLOCK] for g in range(len(absent))]
        if causal is not None:
            pieces[0] = causal(t, pieces[0])
        old = top[:, columns]
        new = old
        for piece, off in zip(pieces, absent):
            new = jnp.maximum(new, jnp.max(piece, axis=0, keepdims=True) - off)
        top[:, columns] = new
        weights = [
            jnp.exp2(piece - (new + off)).astype(jnp.bfloat16)
            for piece, off in zip(pieces, absent)
        ]
        return jnp.exp2(old - new), jnp.concatenate(weights, axis=0)

    def gather(t, fade, weights):
        columns = columns_of(t)
        values = lists[t * TILE // width][1]
        summed = jnp.dot(values, weights, preferred_element_type=jnp.float32)
        mass[:, columns] = mass[:, columns] * fade + summed[DH : DH + 1]
        total[:, columns] = total[:, columns] * fade + summed[:DH]

    scores, held_back = scores_of(0), None
    for t in range(tiles):
        ahead = scores_of(t + 1) if t + 1 < tiles else None
        weighed = weigh(t, scores)
        if held_back is not None:
            gather(t - 1, *held_back)
        scores, held_back = ahead, weighed
    gather(tiles - 1, *held_back)


def penalty(here):
    return jnp.where(here, 0.0, BIG).astype(jnp.float32)


def absorbed(plane, q, z):
    spare = (plane < z) & (z + 1 < q)
    return (plane < q) & (plane - z <= REACH) & (z - plane <= REACH) & ~spare


def attend(
    early, mask_hbm, turned, old_total, old_mass, old_top, k_ref, v_ref, out_ref,
    mask_ref, listed, total, mass, top, held, sent, fetched,
):
    fetch = pltpu.make_async_copy(mask_hbm, mask_ref, fetched.at[0])
    fetch.start()
    tokens = out_ref.shape[0]
    part = min(tokens, BLOCK)
    pieces_here = tokens // part
    width = H * part
    last = mask_ref.shape[1] - 1
    q, c = lax.axis_index("qrow"), lax.axis_index("kcol")
    device = q * lax.axis_size("kcol") + c
    plane_blocks = 2 * lax.axis_size("qrow") * tokens // BLOCK
    firsts = [device * tokens + own * part for own in range(pieces_here)]
    rows = [first // BLOCK for first in firsts]
    state = (turned, total, mass, top)
    total[...] = old_total[...]
    mass[...] = old_mass[...]
    top[...] = old_top[...]

    def gone(block):
        if not early:
            return block < 0
        return absorbed(lax.div(block, plane_blocks), q, c // 2)

    def rows_of(ref, blocks):
        return jnp.concatenate(
            [ref[pl.ds(pl.multiple_of(b * BLOCK, BLOCK), BLOCK), :] for b in blocks], axis=0
        )

    def gathered_list(blocks, absent):
        keys, values = operands(rows_of(k_ref, blocks), rows_of(v_ref, blocks))
        return keys, values, absent

    def causal(t, piece):
        key_at = lax.broadcasted_iota(jnp.int32, piece.shape, 0)
        query_at = lax.broadcasted_iota(jnp.int32, piece.shape, 1) % part
        query_at = query_at + firsts[t * TILE // width] % BLOCK
        return jnp.where(key_at <= query_at, piece, -BIG)

    near = []
    for row in rows:
        blocks = [jnp.maximum(row - back, 0) for back in range(NEAR)]
        absent = [
            penalty((row >= back) & ~gone(block)) for back, block in enumerate(blocks)
        ]
        near.append(gathered_list(blocks, absent))
    attend_to(state, near, width, causal)

    fetch.wait()

    def scan(s, counts):
        lowest = last + 1 - (s + 1) * SCAN

        def note(_, counts):
            found = list(counts)
            for i in reversed(range(SCAN)):
                j = lowest + i
                for own, row in enumerate(rows):
                    listed[own, found[own]] = j
                    far = (j + NEAR <= row).astype(jnp.int32)
                    found[own] = found[own] + far * mask_ref[row, j]
            return tuple(found)

        skip = gone(lowest) | (lowest > rows[-1])
        return lax.fori_loop(0, jnp.where(skip, 0, 1), note, counts)

    counts = lax.fori_loop(
        0, (last + 1) // SCAN, scan, tuple(jnp.int32(0) for _ in rows)
    )
    most = counts[0]
    for count in counts[1:]:
        most = jnp.maximum(most, count)
    done = jnp.int32(0)
    for size, smaller in zip(SIZES, SIZES[1:] + (0,)):
        left = most - done
        trips = jnp.where(left > smaller, (left + size - smaller - 1) // size, 0)

        def step(t, carried, done=done, size=size):
            start = done + t * size
            lists = []
            for own, count in enumerate(counts):
                here = [start + g < count for g in range(size)]
                blocks = [
                    jnp.where(here[g], listed[own, jnp.minimum(start + g, last)], 0)
                    for g in range(size)
                ]
                lists.append(gathered_list(blocks, [penalty(ok) for ok in here]))
            attend_to(state, lists, width)
            return carried

        lax.fori_loop(0, trips, step, 0)
        done = done + trips * size

    copies = []
    for own in range(pieces_here):
        here = pl.ds(own * part, part)
        for h in range(H):
            at = slice(own * width + h * part, own * width + (h + 1) * part)
            there = pl.ds(h * DH, DH)
            held[here, there] = (total[:, at] / mass[:, at]).T
            copy = pltpu.make_async_copy(
                held.at[here, there], out_ref.at[here, there], sent.at[own * H + h]
            )
            copy.start()
            copies.append(copy)
    for copy in copies:
        copy.wait()


def spread(
    q_hbm, k_ref, v_ref, mask_hbm, k_all, v_all, flipped, total, mass, top,
    q_ref, mask_ref, send, recv, shared, local, fetched,
):
    ring, lane = lax.axis_size("kcol"), lax.axis_size("qrow")
    depth, width = ring // 2, lane // 2
    q, c = lax.axis_index("qrow"), lax.axis_index("kcol")
    level, core = c // 2, c % 2
    high, low = q // width, q % width
    tokens = k_ref.shape[0]
    own, whole = (k_ref, v_ref), (k_all, v_all)
    sibling = {"qrow": q, "kcol": level * 2 + (1 - core)}
    over = {"qrow": (1 - high) * width + low, "kcol": c}
    sides = [(low + i) % width for i in range(1, width)]
    beside = [{"qrow": high * width + i, "kcol": c} for i in sides]
    up = {"qrow": q, "kcol": c + 2}
    down = {"qrow": q, "kcol": c - 2}
    has_up, has_down = level < depth - 1, level > 0

    def slot(at, column, parity=core):
        return (at * 2 + parity) * lane + column

    def place(kv, block):
        return whole[kv].at[pl.ds(pl.multiple_of(block * tokens, tokens), tokens), :]

    copies = [
        pltpu.make_async_copy(own[kv], place(kv, slot(level, q)), local.at[kv]) for kv in range(2)
    ]
    for copy in copies:
        copy.start()

    fetches = [
        pltpu.make_async_copy(q_hbm, q_ref, fetched.at[0]),
        pltpu.make_async_copy(mask_hbm, mask_ref, fetched.at[1]),
    ]
    for fetch in fetches:
        fetch.start()

    barrier = pltpu.get_barrier_semaphore()

    def greet(target):
        pl.semaphore_signal(
            barrier, inc=1, device_id=target, device_id_type=pl.DeviceIdType.MESH
        )

    for target in [sibling, over] + beside:
        greet(target)
    pl.when(has_up)(lambda: greet(up))
    pl.when(has_down)(lambda: greet(down))
    ends = has_up.astype(jnp.int32) + has_down.astype(jnp.int32)
    pl.semaphore_wait(barrier, 2 + len(beside) + ends)

    for copy in copies:
        copy.wait()

    final = depth - 1
    mine = q == lane - 1
    over_last = (high == 0) & (low == width - 1)
    over_at, up_at, down_at = 1, 2, 2 + depth
    beside_at = 2 + 2 * depth
    relay_over_at = beside_at + len(beside)
    relay_beside_at = relay_over_at + 1
    lift_at = relay_beside_at + len(beside)
    spare_at = lift_at + 2
    end_over_at = spare_at + depth
    end_beside_at = end_over_at + 2
    end_relay_over_at = end_beside_at + 2 * len(beside)
    end_relay_beside_at = end_relay_over_at + 1

    def beside_last(i):
        return high * width + i == lane - 1

    def end_over(kv):
        return high == 0 if kv == 1 else over_last

    def end_beside(kv, i):
        return i == width - 1 if kv == 0 else beside_last(i)

    def settled(semaphore, rows):
        span = k_all.at[pl.ds(0, rows), :]
        pltpu.make_async_copy(span, span, semaphore).wait()

    def landed(kv, block):
        settled(recv.at[kv, block], tokens)

    def push(kv, block, target, at, arrival=None):
        pltpu.make_async_remote_copy(
            src_ref=place(kv, block),
            dst_ref=place(kv, block),
            send_sem=send.at[at],
            recv_sem=recv.at[kv, block] if arrival is None else arrival,
            device_id=target,
            device_id_type=pl.DeviceIdType.MESH,
        ).start()

    def to_sibling(kv, block, at):
        push(kv, block, sibling, 0, shared.at[at])

    def guarded(ok, body):
        if ok is None:
            body()
        else:
            pl.when(ok)(body)

    def lifted(at):
        return ((at == 0) & (level >= 2)) | ((at == depth - 1) & (level < depth - 2))

    def sent_where(at, way, conditions, body):
        if way <= 0:
            conditions = conditions[:1] + [(at != final) | conditions[1]]
        else:
            conditions = conditions[:1]
        conditions = [c for c in conditions if c is not None]
        if not conditions:
            body()
        else:
            ok = conditions[0]
            for c in conditions[1:]:
                ok &= c
            pl.when(ok)(body)

    def either(at, way, end, usual):
        return jnp.where(at == final, end, usual) if way <= 0 else usual

    def lift(kv, block, at, way):
        if way > 0:
            pl.when((at == 0) & has_up)(lambda: push(kv, block, up, lift_at))
        if way < 0:
            pl.when((at == depth - 1) & has_down)(lambda: push(kv, block, down, lift_at + 1))

    def column_sends(ok, at, way):
        block = slot(at, q)

        def body():
            for kv in range(2):
                if way != 0:
                    landed(kv, block)
                if way >= 0:
                    pl.when(has_up)(lambda: push(kv, block, up, up_at + at))
                if way <= 0:
                    pl.when(has_down)(lambda: push(kv, block, down, down_at + at))
                on_time = None if kv == 1 or way == 0 else ~lifted(at)
                usual = over_at if kv == 1 else spare_at + at
                sent_where(
                    at, way, [on_time, end_over(kv)],
                    lambda: push(kv, block, over, either(at, way, end_over_at + kv, usual)),
                )
                on_time = None if kv == 0 or way == 0 else ~lifted(at)
                for i, (column, target) in enumerate(zip(sides, beside)):
                    usual = beside_at + i if kv == 0 else spare_at + at
                    sent_where(
                        at, way, [on_time, end_beside(kv, column)],
                        lambda: push(
                            kv, block, target,
                            either(at, way, end_beside_at + 2 * i + kv, usual),
                        ),
                    )
                sent_where(at, way, [None, mine], lambda: to_sibling(kv, block, at))

        guarded(ok, body)

    def relays(ok, at, way):
        def body():
            def keys_over():
                for i in sides:
                    block = slot(at, high * width + i)
                    landed(0, block)
                    at_end = end_relay_over_at
                    sent_where(
                        at, way, [None, over_last],
                        lambda: push(0, block, over, either(at, way, at_end, relay_over_at)),
                    )
                    sent_where(at, way, [None, mine], lambda: to_sibling(0, block, at))

            def values_beside():
                block = slot(at, (1 - high) * width + low)
                landed(1, block)
                for i, (column, target) in enumerate(zip(sides, beside)):
                    at_end = end_relay_beside_at + i
                    sent_where(
                        at, way, [None, beside_last(column)],
                        lambda: push(
                            1, block, target, either(at, way, at_end, relay_beside_at + i)
                        ),
                    )
                sent_where(at, way, [None, mine], lambda: to_sibling(1, block, at))

            def rest():
                block = slot(at, (1 - high) * width + low)
                landed(0, block)
                lift(0, block, at, way)
                to_sibling(0, block, at)
                for i in sides:
                    block = slot(at, high * width + i)
                    landed(1, block)
                    lift(1, block, at, way)
                    to_sibling(1, block, at)

            sent_where(at, way, [None, low == width - 1], keys_over)
            sent_where(at, way, [None, high == 1], values_beside)
            sent_where(at, way, [None, mine], rest)

        guarded(ok, body)

    def corners(ok, at, way):
        def body():
            for i in sides:
                block = slot(at, (1 - high) * width + i)
                for kv in range(2):
                    landed(kv, block)
                    to_sibling(kv, block, at)

        if way <= 0:
            needed = (at != final) | mine
            ok = needed if ok is None else ok & needed
        guarded(ok, body)

    def positions(step):
        if step == 0:
            return [(None, level, 0)]
        return [
            (level >= step, level - step, 1),
            (level + step < depth, level + step, -1),
        ]

    state = (flipped, total, mass, top)
    part = min(q_ref.shape[0], BLOCK)
    firsts = [(q * ring + c) * q_ref.shape[0] + own for own in range(0, q_ref.shape[0], part)]
    plane_tokens = 2 * lane * tokens
    half_tokens = plane_tokens // HALVES

    def absorb(step):
        for ok, at, _ in positions(step):
            here = absorbed(at, q, level) if ok is None else ok & absorbed(at, q, level)
            pl.when(here)(lambda at=at: settled(shared.at[at], plane_tokens))

        def half(i, carried):
            plane = jnp.where(i < HALVES, level - step, level + step)
            first = plane * plane_tokens + i % HALVES * half_tokens
            here = pl.ds(pl.multiple_of(first, half_tokens), half_tokens)
            keys, values = operands(k_all[here, :], v_all[here, :])
            lists = []
            for token in firsts:
                absent = [
                    (1 - mask_ref[token // BLOCK, first // BLOCK + g]).astype(jnp.float32) * BIG
                    for g in range(half_tokens // BLOCK)
                ]
                lists.append((keys, values, absent))
            attend_to(state, lists, H * part)
            return carried

        below = (level >= step) & absorbed(level - step, q, level)
        above = (level + step < depth) & (level + step < q) & (step > 0)
        lax.fori_loop(
            jnp.where(below, 0, HALVES), jnp.where(above, 2 * HALVES, HALVES), half, 0
        )

    for step in range(depth + 2):
        if step < depth:
            for ok, at, way in positions(step):
                column_sends(ok, at, way)
        if step == 0:
            for fetch in fetches:
                fetch.wait()
            prepare(q_ref, flipped, total, mass, top)
        if 1 <= step <= depth:
            for ok, at, way in positions(step - 1):
                relays(ok, at, way)
        if step >= 2:
            for ok, at, way in positions(step - 2):
                corners(ok, at, way)
            if step - 2 <= REACH:
                absorb(step - 2)
    for at in range(depth):
        here = ~absorbed(at, q, level)
        if at == final:
            here &= mine
        pl.when(here)(lambda at=at: settled(shared.at[at], plane_tokens))
    pl.when(mine)(lambda: settled(send.at[0], depth * plane_tokens))
    pl.when(~mine)(lambda: settled(send.at[0], final * plane_tokens))
    settled(send.at[over_at], final * tokens)
    settled(send.at[relay_over_at], len(sides) * final * tokens)
    pl.when(over_last)(lambda: settled(send.at[end_relay_over_at], len(sides) * tokens))
    for i, column in enumerate(sides):
        settled(send.at[beside_at + i], final * tokens)
        settled(send.at[relay_beside_at + i], final * tokens)
        pl.when(beside_last(column))(
            lambda i=i: settled(send.at[end_relay_beside_at + i], tokens)
        )
    for kv in range(2):
        on_time = ~lifted(final)
        late = end_over(kv) & on_time if kv == 0 else end_over(kv)
        pl.when(late)(lambda kv=kv: settled(send.at[end_over_at + kv], tokens))
        for i, column in enumerate(sides):
            late = end_beside(kv, column) & on_time if kv == 1 else end_beside(kv, column)
            pl.when(late)(
                lambda i=i, kv=kv: settled(send.at[end_beside_at + 2 * i + kv], tokens)
            )
    lifts = (len(sides) + 1) * tokens
    pl.when(has_up & (level > 0))(lambda: settled(send.at[lift_at], lifts))
    pl.when(has_down & (level < final) & mine)(
        lambda: settled(send.at[lift_at + 1], lifts)
    )
    for at in range(final):
        pl.when(~lifted(at))(
            lambda at=at: settled(send.at[spare_at + at], (1 + len(beside)) * tokens)
        )
    for at in range(depth):
        pl.when(has_up & (level >= at))(lambda at=at: settled(send.at[up_at + at], 2 * tokens))
        pl.when(has_down & (level <= at))(
            lambda at=at: settled(send.at[down_at + at], 2 * tokens)
        )


def in_hbm(array):
    return pltpu.with_memory_space_constraint(array, pltpu.HBM)


def state_of(queries):
    columns = queries.shape[0] * H
    row = jax.ShapeDtypeStruct((1, columns), jnp.float32)
    return (
        jax.ShapeDtypeStruct((2 * DH, columns), jnp.bfloat16),
        jax.ShapeDtypeStruct((DH, columns), jnp.float32),
        row,
        row,
    )


def gathered(queries, keys, values, block_mask):
    ring, lane = lax.axis_size("kcol"), lax.axis_size("qrow")
    devices = ring * lane
    vmem = pl.BlockSpec(memory_space=pltpu.VMEM)
    state = state_of(queries)
    if ring != 2 * lane or lane % 2 or devices > MOST:
        both = ("kcol", "qrow")
        ready = pl.pallas_call(
            prepare, out_shape=state, in_specs=[vmem], out_specs=(vmem,) * len(state)
        )(queries)
        return False, ready, (
            lax.all_gather(keys, both, axis=0, tiled=True),
            lax.all_gather(values, both, axis=0, tiled=True),
        )
    full = jax.ShapeDtypeStruct((keys.shape[0] * devices, keys.shape[1]), keys.dtype)
    side = lane // 2 - 1
    all_keys, all_values, *ready = pl.pallas_call(
        spread,
        out_shape=(full, full) + state,
        in_specs=[pl.BlockSpec(memory_space=pltpu.HBM)] * 4,
        out_specs=(vmem,) * (2 + len(state)),
        scratch_shapes=[
            pltpu.VMEM(queries.shape, queries.dtype),
            pltpu.SMEM(block_mask.shape, jnp.int32),
            pltpu.SemaphoreType.DMA((8 + ring + ring // 2 + 5 * side,)),
            pltpu.SemaphoreType.DMA((2, devices)),
            pltpu.SemaphoreType.DMA((ring // 2,)),
            pltpu.SemaphoreType.DMA((2,)),
            pltpu.SemaphoreType.DMA((2,)),
        ],
        compiler_params=pltpu.CompilerParams(
            collective_id=0, has_side_effects=True, vmem_limit_bytes=40 * 2**20
        ),
    )(in_hbm(queries), in_hbm(keys), in_hbm(values), in_hbm(block_mask))
    return True, ready, (all_keys, all_values)


def shards(queries, keys, values, block_mask):
    early, ready, everything = gathered(queries, keys, values, block_mask)
    vmem = pl.BlockSpec(memory_space=pltpu.VMEM)
    hbm = pl.BlockSpec(memory_space=pltpu.HBM)
    _, *sums = state_of(queries)
    parts = pl.cdiv(queries.shape[0], BLOCK)
    return pl.pallas_call(
        functools.partial(attend, early),
        out_shape=jax.ShapeDtypeStruct(queries.shape, jnp.float32),
        in_specs=[hbm] + [vmem] * 6,
        out_specs=hbm,
        scratch_shapes=[
            pltpu.SMEM(block_mask.shape, jnp.int32),
            pltpu.SMEM((parts, block_mask.shape[1]), jnp.int32),
            *[pltpu.VMEM(s.shape, s.dtype) for s in sums],
            pltpu.VMEM(queries.shape, jnp.float32),
            pltpu.SemaphoreType.DMA((parts * H,)),
            pltpu.SemaphoreType.DMA((1,)),
        ],
        compiler_params=pltpu.CompilerParams(vmem_limit_bytes=48 * 2**20),
    )(in_hbm(block_mask), *ready, *everything)


def solution(mesh):
    placed = (P(("qrow", "kcol"), None), P(("kcol", "qrow"), None), P(("kcol", "qrow"), None), P())
    return jax.shard_map(
        shards, mesh=mesh, in_specs=placed, out_specs=P(("qrow", "kcol"), None), check_vma=False
    )
```
